256 devices in a mesh: zero: 16 (over z, core), cols: 4 (over y), ens: 4 (over x).
Axes of the slice: x: 4, y: 4, z: 8, core: 2. Of those that a mesh axis runs over, the one named last changes fastest.
Arguments:
- weight_gate: float32 [8192, 8192], P(('ens', 'zero'), 'cols'), parts along dimension 0, may hold values from -0.1875 to 0.1875
- moment_gate: float32 [8192, 8192], P(('ens', 'zero'), 'cols'), parts along dimension 0, may hold values from -0.125 to 0.125
- square_gate: float32 [8192, 8192], P(('ens', 'zero'), 'cols'), parts along dimension 0, may hold values from -0.125 to 0.125
- weight_up: float32 [8192, 8192], P(('ens', 'zero'), 'cols'), parts along dimension 0, may hold values from -0.1875 to 0.1875
- moment_up: float32 [8192, 8192], P(('ens', 'zero'), 'cols'), parts along dimension 0, may hold values from -0.125 to 0.125
- square_up: float32 [8192, 8192], P(('ens', 'zero'), 'cols'), parts along dimension 0, may hold values from -0.125 to 0.125
- norm_gain: float32 [8192], P(('ens', 'zero')), parts along dimension 0, may hold values from 0.25 to 1.75
Outputs:
- ready_gate: bfloat16 [8192, 8192], P('ens', 'cols'), parts along dimension 0
- ready_up: bfloat16 [8192, 8192], P('ens', 'cols'), parts along dimension 0
- factor_gate: float32 [32768], P(('ens', 'cols')), parts along dimension 0
- factor_up: float32 [32768], P(('ens', 'cols')), parts along dimension 0
The draws below stay inside these ranges and needn't reach their ends.
There are 4 independent parts, one for each index of `ens`. The reference program is written for one: setup_inputs(seed, part) draws one part's arguments, and reference() takes and returns one part's arrays. A program takes and returns all parts, laid end to end along the dimension named above; each array names one. Nothing has to cross between parts.
All inputs are finite; a program needn't handle non-finite values. Where the reference program divides by a largest or mean magnitude, that divisor is 1e-20 or more.
Results may differ from the reference program's by a relative error of at most 0.001.
Values may be sent and summed in bfloat16 or wider, within the bound.
A program may use at most 128 MiB of HBM per device.

```python
import jax
import jax.numpy as jnp

D_MODEL = 2048
D_INNER = 8192


def raised(array, rng, source, target, parts, factor):
    owner, partner = [(jnp.arange(array.shape[axis_at]) // (array.shape[axis_at] // parts)).reshape([-1 if axis == axis_at else 1 for axis in range(array.ndim)]) for axis_at in (source, target)]
    chosen = jax.random.permutation(rng, parts)[partner]
    strong = (owner == chosen) | (owner == (partner + parts // 2) % parts)
    return jnp.where(strong, factor * array, array)


def steps_of(stream_key, extent, shards, smallest, high):
    loudness = 1.0
    for axis_at, shards_of in shards:
        heights = jax.random.uniform(jax.random.fold_in(jax.random.fold_in(stream_key, 6), axis_at), (shards_of,), jnp.float32, smallest / len(shards), high / len(shards))
        loudness = loudness * jnp.repeat(jnp.exp(heights), extent[axis_at] // shards_of).reshape((-1,) + (1,) * (len(extent) - 1 - axis_at))
    return loudness


def noise(rng, extent, spread, reach, cuts=(), kind=jnp.bfloat16):
    loudness = steps_of(rng, extent, cuts, -0.22, 0.18) if cuts else 1.0
    values = jax.random.normal(rng, extent, jnp.float32) * spread * loudness
    return jnp.minimum(jnp.maximum(values, -reach), reach).astype(kind)


def heavy_noise(own_key, extent, width, most, cuts, heavy, held_as=jnp.bfloat16):
    array = width * jax.random.normal(own_key, extent, jnp.float32)
    if cuts:
        array = array * steps_of(own_key, extent, cuts, -0.22, 0.18)
    return jnp.clip(raised(array, jax.random.fold_in(own_key, 3), *heavy), -most, most).astype(held_as)


def setup_inputs(seed: int = 0, part: int = 0) -> dict:
    keys = jax.random.split(jax.random.key(seed), 8)
    own_keys = jax.random.split(jax.random.fold_in(keys[7], part), 8)
    weight_gate = heavy_noise(own_keys[0], (D_MODEL, D_INNER), D_MODEL ** -0.5, 0.1875, ((0, 16), (1, 4)), (0, 1, 16, 2.0), jnp.float32)
    moment_gate = noise(own_keys[1], (D_MODEL, D_INNER), D_MODEL ** -0.5, 0.125, ((0, 16), (1, 4)), jnp.float32)
    square_gate = noise(own_keys[2], (D_MODEL, D_INNER), D_MODEL ** -0.5, 0.125, ((0, 16), (1, 4)), jnp.float32)
    weight_up = heavy_noise(own_keys[3], (D_MODEL, D_INNER), D_MODEL ** -0.5, 0.1875, ((0, 16), (1, 4)), (0, 1, 16, 2.0), jnp.float32)
    moment_up = noise(own_keys[4], (D_MODEL, D_INNER), D_MODEL ** -0.5, 0.125, ((0, 16), (1, 4)), jnp.float32)
    square_up = noise(own_keys[5], (D_MODEL, D_INNER), D_MODEL ** -0.5, 0.125, ((0, 16), (1, 4)), jnp.float32)
    norm_gain = jnp.clip(1.0 + 0.15 * jax.random.normal(own_keys[6], (D_MODEL,), jnp.float32), 0.25, 1.75)
    return {"weight_gate": weight_gate, "moment_gate": moment_gate, "square_gate": square_gate, "weight_up": weight_up, "moment_up": moment_up, "square_up": square_up, "norm_gain": norm_gain}


learn_rate = 0.2
hold_rate = 0.9


def reference(weight_gate, moment_gate, square_gate, weight_up, moment_up, square_up, norm_gain):
    hold_gate = hold_rate * moment_gate + square_gate
    latest_gate = weight_gate - learn_rate * hold_gate
    hold_up = hold_rate * moment_up + square_up
    latest_up = weight_up - learn_rate * hold_up
    latest_gained_gate = latest_gate * norm_gain[:, None]
    latest_gained_up = latest_up * norm_gain[:, None]
    factor_gate = jnp.max(jnp.abs(latest_gained_gate), axis=0)
    ready_gate = (latest_gained_gate / factor_gate).astype(jnp.bfloat16)
    factor_up = jnp.max(jnp.abs(latest_gained_up), axis=0)
    ready_up = (latest_gained_up / factor_up).astype(jnp.bfloat16)
    return ready_gate, ready_up, factor_gate, factor_up
```

```python
import jax
import jax.numpy as jnp
from jax import lax
from jax.experimental import pallas as pl
from jax.experimental.pallas import tpu as pltpu
from jax.sharding import PartitionSpec as P

learn_rate = 0.2
hold_rate = 0.9
MESH = pl.DeviceIdType.MESH
LANES = 128
GROUP = 1024
PIECE = 512
CW, CCW = 0, 1


def gather_kernel(
    wg, mg, sg, wu, mu, su, gain_ref, out, fac,
    w_buf, m_buf, s_buf, gain_b, mx_own, mx_pair, mx_comb, mx_all, recip,
    load_sem, ring_send, ring_recv, pair_send, pair_recv, mxp_send, mxp_recv, mx_send, mx_recv,
):
    rows, cols = wg.shape
    groups = cols // GROUP
    n_groups = 2 * groups
    per_group = GROUP // PIECE
    n_pieces = n_groups * per_group
    tiles = GROUP // LANES
    chips = lax.axis_size("zero") // 2

    me = lax.axis_index("zero")
    chip, core = me // 2, me % 2

    def peer(step):
        return {"zero": lax.rem(chip + step + 2 * chips, chips) * 2 + core}

    partner = {"zero": chip * 2 + (1 - core)}

    def loads(g):
        a, c = divmod(g, groups)
        span = pl.ds(c * GROUP, GROUP)
        dst = pl.ds(g * GROUP, GROUP)
        srcs = ((wg, mg, sg), (wu, mu, su))[a]
        return [
            pltpu.make_async_copy(src.at[:, span], buf.at[:, dst], load_sem.at[g, i])
            for i, (src, buf) in enumerate(zip(srcs, (w_buf, m_buf, s_buf)))
        ]

    for g in range(n_groups):
        for copy in loads(g):
            copy.start()

    barrier = pltpu.get_barrier_semaphore()
    pl.semaphore_signal(barrier, inc=1, device_id=partner, device_id_type=MESH)
    for step in (4, 3, 5, 2, 6, 1, 7):
        pl.semaphore_signal(barrier, inc=1, device_id=peer(step), device_id_type=MESH)

    gain_b[...] = jnp.broadcast_to(gain_ref[...], (rows, rows)).T

    for g in range(n_groups):
        for copy in loads(g):
            copy.wait()

        def update(j, _, g=g):
            span = pl.ds(pl.multiple_of(g * GROUP + j * LANES, LANES), LANES)
            hold = hold_rate * m_buf[:, span] + s_buf[:, span]
            gained = (w_buf[:, span] - learn_rate * hold) * gain_b[...]
            w_buf[:, span] = gained
            mx_own[g, pl.ds(j, 1), :] = jnp.max(jnp.abs(gained), axis=0, keepdims=True)
            return 0

        lax.fori_loop(0, tiles, update, 0)

    pl.semaphore_wait(barrier, chips)

    pair_max = pltpu.make_async_remote_copy(
        src_ref=mx_own, dst_ref=mx_pair, send_sem=mxp_send, recv_sem=mxp_recv, device_id=partner, device_id_type=MESH
    )
    pair_max.start()
    pair_max.wait()
    mx_comb[...] = jnp.maximum(mx_own[...], mx_pair[...])

    def max_copy(g, step):
        return pltpu.make_async_remote_copy(
            src_ref=mx_comb.at[g], dst_ref=mx_all.at[g, step - 1], send_sem=mx_send.at[g, step - 1],
            recv_sem=mx_recv.at[g, step - 1], device_id=peer(step), device_id_type=MESH,
        )

    for g in range(n_groups):
        for step in (4, 3, 5, 2, 6, 1, 7):
            max_copy(g, step).start()

    def where(owner, k):
        a = k // (n_pieces // 2)
        c = k % (n_pieces // 2)
        return (
            a,
            pl.ds(pl.multiple_of(owner * rows, rows), rows),
            pl.ds(pl.multiple_of(c * PIECE, PIECE), PIECE),
        )

    def ring_copy(way, hop, k):
        owner = lax.rem(chip + (2 * chips - hop if way == CW else hop), chips) * 2 + core
        ref = out.at[where(owner, k)]
        return pltpu.make_async_remote_copy(
            src_ref=ref, dst_ref=ref, send_sem=ring_send.at[way, hop * n_pieces + k],
            recv_sem=ring_recv.at[way, hop * n_pieces + k],
            device_id=peer(1 if way == CW else -1), device_id_type=MESH,
        )

    def ring_wait(way, hop, k):
        ring_copy(way, hop, k).wait_recv()

    def pair_copy(way, hop, k):
        owner = lax.rem(chip + (2 * chips - hop if way == CW else hop), chips) * 2 + core
        ref = out.at[where(owner, k)]
        slot = (way * 4 + hop) * n_pieces + k
        return pltpu.make_async_remote_copy(
            src_ref=ref, dst_ref=ref, send_sem=pair_send.at[slot], recv_sem=pair_recv.at[slot],
            device_id=partner, device_id_type=MESH,
        )

    my_rows = pl.ds(pl.multiple_of(me * rows, rows), rows)
    for g in range(n_groups):
        a, c = divmod(g, groups)
        top = mx_comb[g]
        for step in range(1, chips):
            max_copy(g, step).wait_recv()
            top = jnp.maximum(top, mx_all[g, step - 1])
        fac[a, pl.ds(c * tiles, tiles), :] = top
        recip[...] = 1.0 / top

        for h in range(per_group):

            def scale(j, _, g=g, a=a, c=c, h=h):
                t = h * (PIECE // LANES) + j
                src = pl.ds(pl.multiple_of(g * GROUP + t * LANES, LANES), LANES)
                dst = pl.ds(pl.multiple_of(c * GROUP + t * LANES, LANES), LANES)
                out[a, my_rows, dst] = (w_buf[:, src] * recip[pl.ds(t, 1), :]).astype(jnp.bfloat16)
                return 0

            lax.fori_loop(0, PIECE // LANES, scale, 0)
            k = g * per_group + h
            ring_copy(CW, 0, k).start()
            ring_copy(CCW, 0, k).start()
            pair_copy(CW, 0, k).start()

    def both(i, _):
        hop, k = i // n_pieces, i % n_pieces
        for way in (CW, CCW):
            ring_wait(way, hop, k)
            ring_copy(way, hop + 1, k).start()
            pair_copy(way, hop + 1, k).start()
        return 0

    lax.fori_loop(0, 2 * n_pieces, both, 0)

    def third(i, _):
        for way, k in ((CW, 2 * i), (CCW, 2 * i), (CW, 2 * i + 1), (CCW, 2 * i + 1)):
            ring_wait(way, 2, k)
        for way, k in ((CW, 2 * i), (CCW, 2 * i + 1)):
            ring_copy(way, 3, k).start()
        for way, k in ((CW, 2 * i), (CCW, 2 * i), (CW, 2 * i + 1), (CCW, 2 * i + 1)):
            pair_copy(way, 3, k).start()
        return 0

    lax.fori_loop(0, n_pieces // 2, third, 0)

    def last_pair(way, k):
        owner = lax.rem(chip + chips // 2, chips) * 2 + core
        ref = out.at[where(owner, k)]
        slot = 4 * n_pieces + k
        return pltpu.make_async_remote_copy(
            src_ref=ref, dst_ref=ref, send_sem=pair_send.at[slot], recv_sem=pair_recv.at[slot],
            device_id=partner, device_id_type=MESH,
        )

    def fourth(i, _):
        for way, k in ((CW, 2 * i), (CCW, 2 * i + 1)):
            ring_wait(way, 3, k)
            last_pair(way, k).start()
        return 0

    lax.fori_loop(0, n_pieces // 2, fourth, 0)

    def drain(i, _):
        hop, k = i // n_pieces, i % n_pieces
        for way in (CW, CCW):
            ring_copy(way, hop, k).wait_send()
            pair_copy(way, hop + 1, k).wait()
        return 0

    lax.fori_loop(0, 3 * n_pieces, drain, 0)

    def drain_last(i, _):
        for way, k in ((CW, 2 * i), (CCW, 2 * i + 1)):
            ring_copy(way, 3, k).wait_send()
            last_pair(way, k).wait()
            pair_copy(CW, 0, k).wait()
        return 0

    lax.fori_loop(0, n_pieces // 2, drain_last, 0)
    for g in range(n_groups):
        for step in range(1, chips):
            max_copy(g, step).wait_send()


def write_kernel(full, fac, gate, up, fac_gate, fac_up, sem, fac_sem):
    rows = full.shape[1]
    pieces = sem.shape[1]
    step = rows // pieces

    def copies():
        for a, (dst, small) in enumerate(((gate, fac_gate), (up, fac_up))):
            yield pltpu.make_async_copy(fac.at[a], small, fac_sem.at[a])
            for i in range(pieces):
                span = pl.ds(i * step, step)
                yield pltpu.make_async_copy(full.at[a, span], dst.at[span], sem.at[a, i])

    for copy in copies():
        copy.start()
    for copy in copies():
        copy.wait()


def per_device(weight_gate, moment_gate, square_gate, weight_up, moment_up, square_up, norm_gain):
    rows, cols = weight_gate.shape
    n = lax.axis_size("zero")
    chips = n // 2
    n_groups = 2 * cols // GROUP
    n_pieces = 2 * cols // PIECE
    hbm = pl.BlockSpec(memory_space=pltpu.HBM)
    vmem = pl.BlockSpec(memory_space=pltpu.VMEM)
    stored = (weight_gate, moment_gate, square_gate, weight_up, moment_up, square_up)
    stored = tuple(pltpu.with_memory_space_constraint(x, pltpu.HBM) for x in stored)
    full, fac = pl.pallas_call(
        gather_kernel,
        name="ring",
        out_shape=(
            pltpu.VMEM((2, n * rows, cols), jnp.bfloat16),
            pltpu.VMEM((2, cols // LANES, LANES), jnp.float32),
        ),
        in_specs=[hbm] * 6 + [vmem],
        out_specs=(vmem, vmem),
        scratch_shapes=[
            pltpu.VMEM((rows, 2 * cols), jnp.float32),
            pltpu.VMEM((rows, 2 * cols), jnp.float32),
            pltpu.VMEM((rows, 2 * cols), jnp.float32),
            pltpu.VMEM((rows, LANES), jnp.float32),
            pltpu.VMEM((n_groups, GROUP // LANES, LANES), jnp.float32),
            pltpu.VMEM((n_groups, GROUP // LANES, LANES), jnp.float32),
            pltpu.VMEM((n_groups, GROUP // LANES, LANES), jnp.float32),
            pltpu.VMEM((n_groups, chips - 1, GROUP // LANES, LANES), jnp.float32),
            pltpu.VMEM((GROUP // LANES, LANES), jnp.float32),
            pltpu.SemaphoreType.DMA((n_groups, 3)),
            pltpu.SemaphoreType.DMA((2, 4 * n_pieces)),
            pltpu.SemaphoreType.DMA((2, 4 * n_pieces)),
            pltpu.SemaphoreType.DMA((8 * n_pieces,)),
            pltpu.SemaphoreType.DMA((8 * n_pieces,)),
            pltpu.SemaphoreType.DMA,
            pltpu.SemaphoreType.DMA,
            pltpu.SemaphoreType.DMA((n_groups, chips - 1)),
            pltpu.SemaphoreType.DMA((n_groups, chips - 1)),
        ],
        compiler_params=pltpu.CompilerParams(
            collective_id=0, has_side_effects=True, vmem_limit_bytes=16 * 1024 * 1024
        ),
    )(*stored, norm_gain.reshape(1, rows))
    full, fac = (pltpu.with_memory_space_constraint(x, pltpu.VMEM) for x in (full, fac))
    gate, up, fac_gate, fac_up = pl.pallas_call(
        write_kernel,
        name="write",
        out_shape=(
            jax.ShapeDtypeStruct((n * rows, cols), jnp.bfloat16),
            jax.ShapeDtypeStruct((n * rows, cols), jnp.bfloat16),
            jax.ShapeDtypeStruct((cols // LANES, LANES), jnp.float32),
            jax.ShapeDtypeStruct((cols // LANES, LANES), jnp.float32),
        ),
        in_specs=[pl.BlockSpec(memory_space=pl.ANY)] * 2,
        out_specs=(hbm,) * 4,
        scratch_shapes=[pltpu.SemaphoreType.DMA((2, 8)), pltpu.SemaphoreType.DMA((2,))],
        compiler_params=pltpu.CompilerParams(vmem_limit_bytes=1024 * 1024),
    )(full, fac)
    return gate, up, fac_gate.reshape(cols), fac_up.reshape(cols)


def solution(mesh):
    placed = (P(("ens", "zero"), "cols"),) * 6 + (P(("ens", "zero")),)
    return jax.shard_map(
        per_device,
        mesh=mesh,
        in_specs=placed,
        out_specs=(P("ens", "cols"), P("ens", "cols"), P(("ens", "cols")), P(("ens", "cols"))),
        check_vma=False,
    )
```

```python
import jax
import jax.numpy as jnp
from jax import lax
from jax.experimental import pallas as pl
from jax.experimental.pallas import tpu as pltpu
from jax.sharding import PartitionSpec as P

learn_rate = 0.2
hold_rate = 0.9
MESH = pl.DeviceIdType.MESH
LANES = 128
PIECE = 512
CW, CCW = 0, 1


def gather_kernel(
    wg, mg, sg, wu, mu, su, gain_hbm, out, fac,
    buf, gain_row, gain_b, mx_own, mx_pair, mx_comb, mx_all, mx_first,
    load_sem, gain_sem, ring_send, ring_recv, pair_send, pair_recv, mxp_send, mxp_recv, mx_send, mx_recv,
    first_send, first_recv,
):
    rows, cols = wg.shape
    n_pieces = 2 * cols // PIECE
    tiles = PIECE // LANES
    chips = lax.axis_size("zero") // 2
    far_first = (4, 3, 5, 2, 6, 1, 7)

    me = lax.axis_index("zero")
    chip, core = me // 2, me % 2

    def peer(step, other=False):
        c = 1 - core if other else core
        return {"zero": lax.rem(chip + step + 2 * chips, chips) * 2 + c}

    partner = peer(0, True)

    n_groups = n_pieces // 2

    def loads(k):
        a, c = divmod(k, n_pieces // 2)
        span = pl.ds(c * PIECE, PIECE)
        dst = pl.ds(k * PIECE, PIECE)
        srcs = ((wg, mg, sg), (wu, mu, su))[a]
        return [
            pltpu.make_async_copy(src.at[:, span], buf.at[i, :, dst], load_sem.at[k])
            for i, src in enumerate(srcs)
        ]

    gain_copy = pltpu.make_async_copy(gain_hbm, gain_row, gain_sem)
    gain_copy.start()
    for k in range(n_pieces):
        for copy in loads(k):
            copy.start()

    barrier = pltpu.get_barrier_semaphore()
    for step in far_first:
        for other in (False, True):
            pl.semaphore_signal(barrier, inc=1, device_id=peer(step, other), device_id_type=MESH)
    pl.semaphore_signal(barrier, inc=1, device_id=partner, device_id_type=MESH)

    gain_copy.wait()
    gain_b[...] = jnp.broadcast_to(gain_row[...], (rows, rows)).T

    for k in range(n_pieces):
        landed = buf.at[:, :, pl.ds(k * PIECE, PIECE)]
        pltpu.make_async_copy(landed, landed, load_sem.at[k]).wait()
        for t in range(tiles):
            span = pl.ds(k * PIECE + t * LANES, LANES)
            hold = hold_rate * buf[1, :, span] + buf[2, :, span]
            gained = (buf[0, :, span] - learn_rate * hold) * gain_b[...]
            buf[0, :, span] = gained
            mx_own[k, pl.ds(t, 1), :] = jnp.max(jnp.abs(gained), axis=0, keepdims=True)

    pl.semaphore_wait(barrier, 2 * chips - 1)

    def first_copy(step, other):
        slot = 2 * step + (1 if other else 0) - 1
        return pltpu.make_async_remote_copy(
            src_ref=mx_own.at[0], dst_ref=mx_first.at[slot], send_sem=first_send,
            recv_sem=first_recv, device_id=peer(step, other), device_id_type=MESH,
        )

    direct = [(step, other) for step in far_first for other in (False, True)] + [(0, True)]
    for step, other in direct:
        first_copy(step, other).start()

    pair_max = pltpu.make_async_remote_copy(
        src_ref=mx_own.at[pl.ds(1, n_pieces - 1)], dst_ref=mx_pair, send_sem=mxp_send, recv_sem=mxp_recv,
        device_id=partner, device_id_type=MESH,
    )
    pair_max.start()
    pair_max.wait()
    mx_comb[...] = jnp.maximum(mx_own[1:], mx_pair[...])
    batches = ((0, 1), (1, 2), (3, n_pieces - 4))

    def max_copy(b, step):
        span = pl.ds(*batches[b])
        return pltpu.make_async_remote_copy(
            src_ref=mx_comb.at[span], dst_ref=mx_all.at[step - 1, span], send_sem=mx_send.at[b],
            recv_sem=mx_recv.at[b], device_id=peer(step), device_id_type=MESH,
        )

    for b in range(len(batches)):
        for step in far_first:
            max_copy(b, step).start()

    def block(way, hop, g, half):
        owner = lax.rem(chip + (2 * chips - hop if way == CW else hop), chips) * 2 + core
        width = 2 * PIECE if half is None else PIECE
        start = (g % (n_groups // 2)) * (2 * PIECE) + (half or 0) * PIECE
        rows_of = pl.ds(pl.multiple_of(owner * rows, rows), rows)
        return out.at[g // (n_groups // 2), rows_of, pl.ds(pl.multiple_of(start, PIECE), width)]

    def ring_copy(way, hop, g, half=None):
        ref = block(way, hop, g, half)
        return pltpu.make_async_remote_copy(
            src_ref=ref, dst_ref=ref, send_sem=ring_send.at[way], recv_sem=ring_recv.at[way, hop * n_groups + g],
            device_id=peer(1 if way == CW else -1), device_id_type=MESH,
        )

    def pair_copy(way, hop, g, half=None):
        ref = block(way, hop, g, half)
        return pltpu.make_async_remote_copy(
            src_ref=ref, dst_ref=ref, send_sem=pair_send, recv_sem=pair_recv, device_id=partner, device_id_type=MESH
        )

    my_rows = pl.ds(pl.multiple_of(me * rows, rows), rows)

    def send_own(k, top):
        a, c = divmod(k, n_pieces // 2)
        fac[a, pl.ds(c * tiles, tiles), :] = top
        recip = 1.0 / top
        for t in range(tiles):
            src = pl.ds(k * PIECE + t * LANES, LANES)
            dst = pl.ds(c * PIECE + t * LANES, LANES)
            out[a, my_rows, dst] = (buf[0, :, src] * recip[t : t + 1]).astype(jnp.bfloat16)
        g, half = divmod(k, 2)
        ring_copy(CW, 0, g, half).start()
        ring_copy(CCW, 0, g, half).start()
        pair_copy(CW, 0, g, half).start()

    top = mx_own[0]
    pltpu.make_async_copy(mx_first, mx_first, first_recv).wait()
    for slot in range(2 * chips - 1):
        top = jnp.maximum(top, mx_first[slot])
    send_own(0, top)
    for b, (start, size) in enumerate(batches):
        came = mx_all.at[:, pl.ds(start, size)]
        pltpu.make_async_copy(came, came, mx_recv.at[b]).wait()
        for k in range(start, start + size):
            top = mx_comb[k]
            for step in far_first:
                top = jnp.maximum(top, mx_all[step - 1, k])
            send_own(k + 1, top)

    def both(i, _):
        hop, g = i // n_groups, i % n_groups
        for way in (CW, CCW):
            ring_copy(way, hop, g).wait_recv()
            ring_copy(way, hop + 1, g).start()
            pair_copy(way, hop + 1, g).start()
        return 0

    lax.fori_loop(0, 2 * n_groups, both, 0)

    def third(g, _):
        for way in (CW, CCW):
            ring_copy(way, 2, g).wait_recv()
            ring_copy(way, 3, g, way).start()
            pair_copy(way, 3, g).start()
        return 0

    lax.fori_loop(0, n_groups, third, 0)

    def fourth(g, _):
        for way in (CW, CCW):
            ring_copy(way, 3, g, way).wait_recv()
            pair_copy(way, 4, g, way).start()
        return 0

    lax.fori_loop(0, n_groups, fourth, 0)

    theirs = out.at[:, pl.ds(0, chips * rows)]
    pltpu.make_async_copy(theirs, theirs, pair_send).wait()
    pltpu.make_async_copy(theirs, theirs, pair_recv).wait()
    for way in (CW, CCW):
        sent = out.at[0, pl.ds(0, (chips - 1) * rows)]
        pltpu.make_async_copy(sent, sent, ring_send.at[way]).wait()
    pltpu.make_async_copy(mx_first, mx_first, first_send).wait()
    for b, (start, size) in enumerate(batches):
        came = mx_all.at[:, pl.ds(start, size)]
        pltpu.make_async_copy(came, came, mx_send.at[b]).wait()


def write_kernel(full, fac, gate, up, fac_gate, fac_up, sem):
    step = full.shape[1] // 8
    smalls = [pltpu.make_async_copy(fac.at[a], dst, sem.at[2 + a]) for a, dst in enumerate((fac_gate, fac_up))]
    for a, dst in enumerate((gate, up)):
        for i in range(8):
            span = pl.ds(i * step, step)
            pltpu.make_async_copy(full.at[a, span], dst.at[span], sem.at[a]).start()
    for small in smalls:
        small.start()
    for a, dst in enumerate((gate, up)):
        pltpu.make_async_copy(full.at[a], dst, sem.at[a]).wait()
    for small in smalls:
        small.wait()


def per_device(weight_gate, moment_gate, square_gate, weight_up, moment_up, square_up, norm_gain):
    rows, cols = weight_gate.shape
    n = lax.axis_size("zero")
    chips = n // 2
    n_pieces = 2 * cols // PIECE
    tiles = PIECE // LANES
    hbm = pl.BlockSpec(memory_space=pltpu.HBM)
    vmem = pl.BlockSpec(memory_space=pltpu.VMEM)
    stored = (weight_gate, moment_gate, square_gate, weight_up, moment_up, square_up, norm_gain.reshape(1, rows))
    stored = tuple(pltpu.with_memory_space_constraint(x, pltpu.HBM) for x in stored)
    full, fac = pl.pallas_call(
        gather_kernel,
        name="ring",
        out_shape=(
            pltpu.VMEM((2, n * rows, cols), jnp.bfloat16),
            pltpu.VMEM((2, cols // LANES, LANES), jnp.float32),
        ),
        in_specs=[hbm] * 7,
        out_specs=(vmem, vmem),
        scratch_shapes=[
            pltpu.VMEM((3, rows, 2 * cols), jnp.float32),
            pltpu.VMEM((1, rows), jnp.float32),
            pltpu.VMEM((rows, rows), jnp.float32),
            pltpu.VMEM((n_pieces, tiles, LANES), jnp.float32),
            pltpu.VMEM((n_pieces - 1, tiles, LANES), jnp.float32),
            pltpu.VMEM((n_pieces - 1, tiles, LANES), jnp.float32),
            pltpu.VMEM((chips - 1, n_pieces - 1, tiles, LANES), jnp.float32),
            pltpu.VMEM((n - 1, tiles, LANES), jnp.float32),
            pltpu.SemaphoreType.DMA((n_pieces,)),
            pltpu.SemaphoreType.DMA,
            pltpu.SemaphoreType.DMA((2,)),
            pltpu.SemaphoreType.DMA((2, 2 * n_pieces)),
            pltpu.SemaphoreType.DMA,
            pltpu.SemaphoreType.DMA,
            pltpu.SemaphoreType.DMA,
            pltpu.SemaphoreType.DMA,
            pltpu.SemaphoreType.DMA((3,)),
            pltpu.SemaphoreType.DMA((3,)),
            pltpu.SemaphoreType.DMA,
            pltpu.SemaphoreType.DMA,
        ],
        compiler_params=pltpu.CompilerParams(
            collective_id=0, has_side_effects=True, vmem_limit_bytes=16 * 1024 * 1024
        ),
    )(*stored)
    full, fac = (pltpu.with_memory_space_constraint(x, pltpu.VMEM) for x in (full, fac))
    gate, up, fac_gate, fac_up = pl.pallas_call(
        write_kernel,
        name="write",
        out_shape=(
            jax.ShapeDtypeStruct((n * rows, cols), jnp.bfloat16),
            jax.ShapeDtypeStruct((n * rows, cols), jnp.bfloat16),
            jax.ShapeDtypeStruct((cols // LANES, LANES), jnp.float32),
            jax.ShapeDtypeStruct((cols // LANES, LANES), jnp.float32),
        ),
        in_specs=[pl.BlockSpec(memory_space=pl.ANY)] * 2,
        out_specs=(hbm,) * 4,
        scratch_shapes=[pltpu.SemaphoreType.DMA((4,))],
        compiler_params=pltpu.CompilerParams(vmem_limit_bytes=1024 * 1024),
    )(full, fac)
    return gate, up, fac_gate.reshape(cols), fac_up.reshape(cols)


def solution(mesh):
    placed = (P(("ens", "zero"), "cols"),) * 6 + (P(("ens", "zero")),)
    return jax.shard_map(
        per_device,
        mesh=mesh,
        in_specs=placed,
        out_specs=(P("ens", "cols"), P("ens", "cols"), P(("ens", "cols")), P(("ens", "cols"))),
        check_vma=False,
    )
```

```python
import jax
import jax.numpy as jnp
from jax import lax
from jax.experimental import pallas as pl
from jax.experimental.pallas import tpu as pltpu
from jax.sharding import PartitionSpec as P

learn_rate = 0.2
hold_rate = 0.9
MESH = pl.DeviceIdType.MESH
LANES = 128
PIECE = 512
EARLY = 256
CW, CCW = 0, 1


def gather_kernel(
    wg, mg, sg, wu, mu, su, gain_hbm, out, fac,
    buf, gain_row, gain_b, mx_own, mx_pair, mx_comb, mx_all, mx_first, mx_final, early,
    load_sem, gain_sem, ring_send, ring_recv, pair_recv, mxp_send, mxp_recv, mx_send, mx_recv,
    first_send, first_recv, final_send, final_recv, early_send, early_recv,
):
    rows, cols = wg.shape
    n_pieces = 2 * cols // PIECE
    tiles = PIECE // LANES
    chips = lax.axis_size("zero") // 2
    far_first = (4, 3, 5, 2, 6, 1, 7)

    me = lax.axis_index("zero")
    chip, core = me // 2, me % 2

    def peer(step, other=False):
        c = 1 - core if other else core
        return {"zero": lax.rem(chip + step + 2 * chips, chips) * 2 + c}

    partner = peer(0, True)

    n_groups = n_pieces // 2

    def loads(k):
        a, c = divmod(k, n_pieces // 2)
        span = pl.ds(c * PIECE, PIECE)
        dst = pl.ds(k * PIECE, PIECE)
        srcs = ((wg, mg, sg), (wu, mu, su))[a]
        return [
            pltpu.make_async_copy(src.at[:, span], buf.at[i, :, dst], load_sem.at[k])
            for i, src in enumerate(srcs)
        ]

    gain_copy = pltpu.make_async_copy(gain_hbm, gain_row, gain_sem)
    gain_copy.start()
    for k in range(n_pieces):
        for copy in loads(k):
            copy.start()

    barrier = pltpu.get_barrier_semaphore()
    for step in far_first:
        for other in (False, True):
            pl.semaphore_signal(barrier, inc=1, device_id=peer(step, other), device_id_type=MESH)
    pl.semaphore_signal(barrier, inc=1, device_id=partner, device_id_type=MESH)

    gain_copy.wait()
    gain_b[...] = jnp.broadcast_to(gain_row[...], (rows, rows)).T

    for k in range(n_pieces):
        landed = buf.at[:, :, pl.ds(k * PIECE, PIECE)]
        pltpu.make_async_copy(landed, landed, load_sem.at[k]).wait()
        for t in range(tiles):
            span = pl.ds(k * PIECE + t * LANES, LANES)
            hold = hold_rate * buf[1, :, span] + buf[2, :, span]
            gained = (buf[0, :, span] - learn_rate * hold) * gain_b[...]
            buf[0, :, span] = gained
            mx_own[k, pl.ds(t, 1), :] = jnp.max(jnp.abs(gained), axis=0, keepdims=True)

    pl.semaphore_wait(barrier, 2 * chips - 1)

    def first_copy(step, other):
        slot = 2 * step + (1 if other else 0) - 1
        return pltpu.make_async_remote_copy(
            src_ref=mx_own.at[0], dst_ref=mx_first.at[slot], send_sem=first_send,
            recv_sem=first_recv, device_id=peer(step, other), device_id_type=MESH,
        )

    direct = [(step, other) for step in far_first for other in (False, True)] + [(0, True)]
    for step, other in direct:
        first_copy(step, other).start()

    share = n_pieces // 2
    mine, theirs = core * share, (1 - core) * share
    last = theirs + share - 1
    early_from = pl.multiple_of(last * PIECE + PIECE - EARLY, LANES)

    def early_copy(way):
        return pltpu.make_async_remote_copy(
            src_ref=buf.at[0, :, pl.ds(early_from, EARLY)], dst_ref=early.at[way], send_sem=early_send,
            recv_sem=early_recv.at[way], device_id=peer(1 if way == CW else -1), device_id_type=MESH,
        )

    for way in (CW, CCW):
        early_copy(way).start()

    pair_max = pltpu.make_async_remote_copy(
        src_ref=mx_own.at[pl.ds(theirs, share)], dst_ref=mx_pair, send_sem=mxp_send, recv_sem=mxp_recv,
        device_id=partner, device_id_type=MESH,
    )
    pair_max.start()
    pair_max.wait()
    mx_comb[...] = jnp.maximum(mx_own[pl.ds(mine, share)], mx_pair[...])
    batch = 2
    n_batches = share // batch

    def max_copy(b, step):
        span = pl.ds(b * batch, batch)
        return pltpu.make_async_remote_copy(
            src_ref=mx_comb.at[span], dst_ref=mx_all.at[step - 1, span], send_sem=mx_send,
            recv_sem=mx_recv.at[b], device_id=peer(step), device_id_type=MESH,
        )

    for b in range(n_batches):
        for step in far_first:
            max_copy(b, step).start()

    def part(way, hop, g, start, width):
        owner = lax.rem(chip + (2 * chips - hop if way == CW else hop), chips) * 2 + core
        start = (g % (n_groups // 2)) * (2 * PIECE) + start
        rows_of = pl.ds(pl.multiple_of(owner * rows, rows), rows)
        return out.at[g // (n_groups // 2), rows_of, pl.ds(pl.multiple_of(start, LANES), width)]

    def ring_copy(way, hop, i, g, start=0, width=2 * PIECE):
        ref = part(way, hop, g, start, width)
        slot = hop * 2 + i // 2 if width == 2 * PIECE or hop == 0 else 6 + i
        return pltpu.make_async_remote_copy(
            src_ref=ref, dst_ref=ref, send_sem=ring_send, recv_sem=ring_recv.at[way, slot],
            device_id=peer(1 if way == CW else -1), device_id_type=MESH,
        )

    def pair_copy(way, hop, g, start=0, width=2 * PIECE):
        ref = part(way, hop, g, start, width)
        return pltpu.make_async_remote_copy(
            src_ref=ref, dst_ref=ref, send_sem=ring_send, recv_sem=pair_recv, device_id=partner, device_id_type=MESH
        )

    def turn(i):
        return lax.rem(i + core * (n_groups // 2), n_groups)

    def send_own(k, i, half, top, width=PIECE):
        recip = 1.0 / top
        a, c = k // share, k % share
        for t in range(tiles):
            src = pl.ds(pl.multiple_of(k * PIECE + t * LANES, LANES), LANES)
            dst = pl.ds(pl.multiple_of(c * PIECE + t * LANES, LANES), LANES)
            rows_of = pl.ds(pl.multiple_of(me * rows, rows), rows)
            out[a, rows_of, dst] = (buf[0, :, src] * recip[t : t + 1]).astype(jnp.bfloat16)
        g = k // 2
        ring_copy(CW, 0, i, g, half * PIECE, width).start()
        ring_copy(CCW, 0, i, g, half * PIECE, width).start()
        pair_copy(CW, 0, g, half * PIECE, PIECE).start()

    top = mx_own[0]
    pltpu.make_async_copy(mx_first, mx_first, first_recv).wait()
    for slot in range(2 * chips - 1):
        top = jnp.maximum(top, mx_first[slot])
    send_own(0, core * (n_groups // 2), 0, top)

    def final_copy(b):
        ref = mx_final.at[pl.ds(mine + b * batch, batch)]
        return pltpu.make_async_remote_copy(
            src_ref=ref, dst_ref=ref, send_sem=final_send, recv_sem=final_recv.at[b],
            device_id=partner, device_id_type=MESH,
        )

    for b in range(n_batches):
        span = pl.ds(b * batch, batch)
        came = mx_all.at[:, span]
        pltpu.make_async_copy(came, came, mx_recv.at[b]).wait()
        top = mx_comb[span]
        for step in far_first:
            top = jnp.maximum(top, mx_all[step - 1, span])
        mx_final[pl.ds(mine + b * batch, batch)] = top
        final_copy(b).start()
        for h in range(batch):
            if b == 0 and h == 0:

                @pl.when(core == 1)
                def _(top=top[0]):
                    send_own(mine, 0, 0, top)

            else:
                send_own(mine + b * batch + h, b, h, top[h])

    for b in range(n_batches):
        came = mx_final.at[pl.ds(theirs + b * batch, batch)]
        pltpu.make_async_copy(came, came, final_recv.at[b]).wait()
        for h in range(batch):
            k = theirs + b * batch + h
            if b == 0 and h == 0:

                @pl.when(core == 0)
                def _(k=k):
                    send_own(k, n_groups // 2, 0, mx_final[k])

            else:
                is_last = b == n_batches - 1 and h == batch - 1
                send_own(k, n_groups // 2 + b, h, mx_final[k], PIECE - EARLY if is_last else PIECE)

    for k in range(n_pieces):
        a, c = divmod(k, share)
        fac[a, pl.ds(c * tiles, tiles), :] = mx_final[k]

    def landed(way, hop, pair):
        ref = out.at[0, pl.ds(0, rows), pl.ds(0, 4 * PIECE)]
        pltpu.make_async_copy(ref, ref, ring_recv.at[way, hop * 2 + pair]).wait()

    def onward(way, hop, pair):
        for i in (2 * pair, 2 * pair + 1):
            g = turn(i)
            ring_copy(way, hop + 1, i, g).start()
            pair_copy(way, hop + 1, g).start()

    for way in (CW, CCW):
        landed(way, 0, 0)
        onward(way, 0, 0)

    recip = 1.0 / mx_final[last]
    for way in (CW, CCW):
        ref = out.at[0, pl.ds(0, rows - rows * EARLY // (4 * PIECE)), pl.ds(0, 4 * PIECE)]
        pltpu.make_async_copy(ref, ref, ring_recv.at[way, 1]).wait()
        early_copy(way).wait_recv()
        owner = lax.rem(chip + (chips - 1 if way == CW else 1), chips) * 2 + core
        rows_of = pl.ds(pl.multiple_of(owner * rows, rows), rows)
        for t in range(EARLY // LANES):
            column = (last % share) * PIECE + PIECE - EARLY + t * LANES
            factor = recip[tiles - EARLY // LANES + t : tiles - EARLY // LANES + t + 1]
            scaled = early[way, :, pl.ds(t * LANES, LANES)] * factor
            out[last // share, rows_of, pl.ds(pl.multiple_of(column, LANES), LANES)] = scaled.astype(jnp.bfloat16)
        onward(way, 0, 1)

    for pair in range(2):
        for way in (CW, CCW):
            landed(way, 1, pair)
            onward(way, 1, pair)

    for pair in range(2):
        for way in (CW, CCW):
            landed(way, 2, pair)
            for i in (2 * pair, 2 * pair + 1):
                g = turn(i)
                ring_copy(way, 3, i, g, way * PIECE, PIECE).start()
                pair_copy(way, 3, g).start()

    def fourth(i, _):
        g = turn(i)
        for way in (CW, CCW):
            ring_copy(way, 3, i, g, way * PIECE, PIECE).wait_recv()
            pair_copy(way, 4, g, way * PIECE, PIECE).start()
        return 0

    lax.fori_loop(0, n_groups, fourth, 0)

    handed = out.at[:, pl.ds(0, chips * rows)]
    pltpu.make_async_copy(handed, handed, pair_recv).wait()
    sent = out.at[:, pl.ds(0, (2 * chips - 1) * rows - rows * EARLY // cols)]
    pltpu.make_async_copy(sent, sent, ring_send).wait()
    pltpu.make_async_copy(early, early, early_send).wait()
    pltpu.make_async_copy(mx_first, mx_first, first_send).wait()
    pltpu.make_async_copy(mx_all, mx_all, mx_send).wait()
    pltpu.make_async_copy(mx_pair, mx_pair, final_send).wait()


def write_kernel(full, fac, gate, up, fac_gate, fac_up, sem):
    step = full.shape[1] // 8
    smalls = [pltpu.make_async_copy(fac.at[a], dst, sem.at[2 + a]) for a, dst in enumerate((fac_gate, fac_up))]
    for a, dst in enumerate((gate, up)):
        for i in range(8):
            span = pl.ds(i * step, step)
            pltpu.make_async_copy(full.at[a, span], dst.at[span], sem.at[a]).start()
    for small in smalls:
        small.start()
    for a, dst in enumerate((gate, up)):
        pltpu.make_async_copy(full.at[a], dst, sem.at[a]).wait()
    for small in smalls:
        small.wait()


def per_device(weight_gate, moment_gate, square_gate, weight_up, moment_up, square_up, norm_gain):
    rows, cols = weight_gate.shape
    n = lax.axis_size("zero")
    chips = n // 2
    n_pieces = 2 * cols // PIECE
    tiles = PIECE // LANES
    hbm = pl.BlockSpec(memory_space=pltpu.HBM)
    vmem = pl.BlockSpec(memory_space=pltpu.VMEM)
    stored = (weight_gate, moment_gate, square_gate, weight_up, moment_up, square_up, norm_gain.reshape(1, rows))
    stored = tuple(pltpu.with_memory_space_constraint(x, pltpu.HBM) for x in stored)
    full, fac = pl.pallas_call(
        gather_kernel,
        name="ring",
        out_shape=(
            pltpu.VMEM((2, n * rows, cols), jnp.bfloat16),
            pltpu.VMEM((2, cols // LANES, LANES), jnp.float32),
        ),
        in_specs=[hbm] * 7,
        out_specs=(vmem, vmem),
        scratch_shapes=[
            pltpu.VMEM((3, rows, 2 * cols), jnp.float32),
            pltpu.VMEM((1, rows), jnp.float32),
            pltpu.VMEM((rows, rows), jnp.float32),
            pltpu.VMEM((n_pieces, tiles, LANES), jnp.float32),
            pltpu.VMEM((n_pieces // 2, tiles, LANES), jnp.float32),
            pltpu.VMEM((n_pieces // 2, tiles, LANES), jnp.float32),
            pltpu.VMEM((chips - 1, n_pieces // 2, tiles, LANES), jnp.float32),
            pltpu.VMEM((n - 1, tiles, LANES), jnp.float32),
            pltpu.VMEM((n_pieces, tiles, LANES), jnp.float32),
            pltpu.VMEM((2, rows, EARLY), jnp.float32),
            pltpu.SemaphoreType.DMA((n_pieces,)),
            pltpu.SemaphoreType.DMA,
            pltpu.SemaphoreType.DMA,
            pltpu.SemaphoreType.DMA((2, 10)),
            pltpu.SemaphoreType.DMA,
            pltpu.SemaphoreType.DMA,
            pltpu.SemaphoreType.DMA,
            pltpu.SemaphoreType.DMA,
            pltpu.SemaphoreType.DMA((2,)),
            pltpu.SemaphoreType.DMA,
            pltpu.SemaphoreType.DMA,
            pltpu.SemaphoreType.DMA,
            pltpu.SemaphoreType.DMA((2,)),
            pltpu.SemaphoreType.DMA,
            pltpu.SemaphoreType.DMA((2,)),
        ],
        compiler_params=pltpu.CompilerParams(
            collective_id=0, has_side_effects=True, vmem_limit_bytes=16 * 1024 * 1024
        ),
    )(*stored)
    full, fac = (pltpu.with_memory_space_constraint(x, pltpu.VMEM) for x in (full, fac))
    gate, up, fac_gate, fac_up = pl.pallas_call(
        write_kernel,
        name="write",
        out_shape=(
            jax.ShapeDtypeStruct((n * rows, cols), jnp.bfloat16),
            jax.ShapeDtypeStruct((n * rows, cols), jnp.bfloat16),
            jax.ShapeDtypeStruct((cols // LANES, LANES), jnp.float32),
            jax.ShapeDtypeStruct((cols // LANES, LANES), jnp.float32),
        ),
        in_specs=[pl.BlockSpec(memory_space=pl.ANY)] * 2,
        out_specs=(hbm,) * 4,
        scratch_shapes=[pltpu.SemaphoreType.DMA((4,))],
        compiler_params=pltpu.CompilerParams(vmem_limit_bytes=1024 * 1024),
    )(full, fac)
    return gate, up, fac_gate.reshape(cols), fac_up.reshape(cols)


def solution(mesh):
    placed = (P(("ens", "zero"), "cols"),) * 6 + (P(("ens", "zero")),)
    return jax.shard_map(
        per_device,
        mesh=mesh,
        in_specs=placed,
        out_specs=(P("ens", "cols"), P("ens", "cols"), P(("ens", "cols")), P(("ens", "cols"))),
        check_vma=False,
    )
```

```python
import jax
import jax.numpy as jnp
from jax import lax
from jax.experimental import pallas as pl
from jax.experimental.pallas import tpu as pltpu
from jax.sharding import PartitionSpec as P

learn_rate = 0.2
hold_rate = 0.9
MESH = pl.DeviceIdType.MESH
LANES = 128
PIECE = 512
EARLY = 256
CW, CCW = 0, 1


def gather_kernel(
    wg, mg, sg, wu, mu, su, gain_hbm, out, fac,
    buf, gain_row, gain_b, mx_own, mx_pair, mx_comb, mx_all, mx_first, mx_final, early,
    load_sem, gain_sem, ring_send, ring_recv, pair_recv, mxp_send, mxp_recv, mx_send, mx_recv,
    first_send, first_recv, final_send, final_recv, early_send, early_recv, hand_recv, relay_recv,
):
    rows, cols = wg.shape
    n_pieces = 2 * cols // PIECE
    tiles = PIECE // LANES
    chips = lax.axis_size("zero") // 2
    far_first = (4, 3, 5, 2, 6, 1, 7)

    me = lax.axis_index("zero")
    chip, core = me // 2, me % 2

    def peer(step, other=False):
        c = 1 - core if other else core
        return {"zero": lax.rem(chip + step + 2 * chips, chips) * 2 + c}

    partner = peer(0, True)

    n_groups = n_pieces // 2

    def loads(k):
        a, c = divmod(k, n_pieces // 2)
        span = pl.ds(c * PIECE, PIECE)
        dst = pl.ds(k * PIECE, PIECE)
        srcs = ((wg, mg, sg), (wu, mu, su))[a]
        return [
            pltpu.make_async_copy(src.at[:, span], buf.at[i, :, dst], load_sem.at[k])
            for i, src in enumerate(srcs)
        ]

    gain_copy = pltpu.make_async_copy(gain_hbm, gain_row, gain_sem)
    gain_copy.start()
    for k in range(n_pieces):
        for copy in loads(k):
            copy.start()

    barrier = pltpu.get_barrier_semaphore()
    for step in far_first:
        for other in (False, True):
            pl.semaphore_signal(barrier, inc=1, device_id=peer(step, other), device_id_type=MESH)
    pl.semaphore_signal(barrier, inc=1, device_id=partner, device_id_type=MESH)

    gain_copy.wait()
    gain_b[...] = jnp.broadcast_to(gain_row[...], (rows, rows)).T

    for k in range(n_pieces):
        landed = buf.at[:, :, pl.ds(k * PIECE, PIECE)]
        pltpu.make_async_copy(landed, landed, load_sem.at[k]).wait()
        for t in range(tiles):
            span = pl.ds(k * PIECE + t * LANES, LANES)
            hold = hold_rate * buf[1, :, span] + buf[2, :, span]
            gained = (buf[0, :, span] - learn_rate * hold) * gain_b[...]
            buf[0, :, span] = gained
            mx_own[k, pl.ds(t, 1), :] = jnp.max(jnp.abs(gained), axis=0, keepdims=True)

    pl.semaphore_wait(barrier, 2 * chips - 1)

    def first_copy(step, other):
        slot = 2 * step + (1 if other else 0) - 1
        return pltpu.make_async_remote_copy(
            src_ref=mx_own.at[0], dst_ref=mx_first.at[slot], send_sem=first_send,
            recv_sem=first_recv, device_id=peer(step, other), device_id_type=MESH,
        )

    direct = [(step, other) for step in far_first for other in (False, True)] + [(0, True)]
    for step, other in direct:
        first_copy(step, other).start()

    share = n_pieces // 2
    mine, theirs = core * share, (1 - core) * share
    last = theirs + share - 1
    early_from = pl.multiple_of(last * PIECE + PIECE - EARLY, LANES)

    def early_copy(way, start, size):
        span = pl.ds(start, size)
        return pltpu.make_async_remote_copy(
            src_ref=buf.at[0, span, pl.ds(early_from, EARLY)], dst_ref=early.at[way, span], send_sem=early_send,
            recv_sem=early_recv.at[way], device_id=peer(1 if way == CW else -1), device_id_type=MESH,
        )

    for way in (CW, CCW):
        early_copy(way, 0, 64).start()

    pair_max = pltpu.make_async_remote_copy(
        src_ref=mx_own.at[pl.ds(theirs, share)], dst_ref=mx_pair, send_sem=mxp_send, recv_sem=mxp_recv,
        device_id=partner, device_id_type=MESH,
    )
    pair_max.start()
    pair_max.wait()
    mx_comb[...] = jnp.maximum(mx_own[pl.ds(mine, share)], mx_pair[...])
    batch = 2
    n_batches = share // batch

    def max_copy(b, step):
        span = pl.ds(b * batch, batch)
        return pltpu.make_async_remote_copy(
            src_ref=mx_comb.at[span], dst_ref=mx_all.at[step - 1, span], send_sem=mx_send,
            recv_sem=mx_recv.at[b], device_id=peer(step), device_id_type=MESH,
        )

    for b in range(n_batches):
        for step in far_first:
            max_copy(b, step).start()
    for way in (CW, CCW):
        early_copy(way, 64, rows - 64).start()

    def part(way, hop, g, start, width):
        owner = lax.rem(chip + (2 * chips - hop if way == CW else hop), chips) * 2 + core
        start = (g % (n_groups // 2)) * (2 * PIECE) + start
        rows_of = pl.ds(pl.multiple_of(owner * rows, rows), rows)
        return out.at[g // (n_groups // 2), rows_of, pl.ds(pl.multiple_of(start, LANES), width)]

    def ring_copy(way, hop, i, g, start=0, width=2 * PIECE):
        ref = part(way, hop, g, start, width)
        slot = hop * 2 + i // 2 if width == 2 * PIECE or hop == 0 else 6 + i
        return pltpu.make_async_remote_copy(
            src_ref=ref, dst_ref=ref, send_sem=ring_send, recv_sem=ring_recv.at[way, slot],
            device_id=peer(1 if way == CW else -1), device_id_type=MESH,
        )

    def pair_copy(way, hop, g, start=0, width=2 * PIECE):
        ref = part(way, hop, g, start, width)
        return pltpu.make_async_remote_copy(
            src_ref=ref, dst_ref=ref, send_sem=ring_send, recv_sem=pair_recv, device_id=partner, device_id_type=MESH
        )

    def turn(i):
        return lax.rem(i + core * (n_groups // 2), n_groups)

    def send_own(k, i, half, top, width=PIECE):
        recip = 1.0 / top
        a, c = k // share, k % share
        for t in range(tiles):
            src = pl.ds(pl.multiple_of(k * PIECE + t * LANES, LANES), LANES)
            dst = pl.ds(pl.multiple_of(c * PIECE + t * LANES, LANES), LANES)
            rows_of = pl.ds(pl.multiple_of(me * rows, rows), rows)
            out[a, rows_of, dst] = (buf[0, :, src] * recip[t : t + 1]).astype(jnp.bfloat16)
        g = k // 2
        ring_copy(CW, 0, i, g, half * PIECE, width).start()
        ring_copy(CCW, 0, i, g, half * PIECE, width).start()
        pair_copy(CW, 0, g, half * PIECE, PIECE).start()

    top = mx_own[0]
    pltpu.make_async_copy(mx_first, mx_first, first_recv).wait()
    for slot in range(2 * chips - 1):
        top = jnp.maximum(top, mx_first[slot])
    send_own(0, core * (n_groups // 2), 0, top)

    def final_copy(b):
        ref = mx_final.at[pl.ds(mine + b * batch, batch)]
        return pltpu.make_async_remote_copy(
            src_ref=ref, dst_ref=ref, send_sem=final_send, recv_sem=final_recv.at[b],
            device_id=partner, device_id_type=MESH,
        )

    for b in range(n_batches):
        span = pl.ds(b * batch, batch)
        came = mx_all.at[:, span]
        pltpu.make_async_copy(came, came, mx_recv.at[b]).wait()
        top = mx_comb[span]
        for step in far_first:
            top = jnp.maximum(top, mx_all[step - 1, span])
        mx_final[pl.ds(mine + b * batch, batch)] = top
        final_copy(b).start()
        for h in range(batch):
            if b == 0 and h == 0:

                @pl.when(core == 1)
                def _(top=top[0]):
                    send_own(mine, 0, 0, top)

            else:
                send_own(mine + b * batch + h, b, h, top[h])

    for b in range(n_batches):
        came = mx_final.at[pl.ds(theirs + b * batch, batch)]
        pltpu.make_async_copy(came, came, final_recv.at[b]).wait()
        for h in range(batch):
            k = theirs + b * batch + h
            if b == 0 and h == 0:

                @pl.when(core == 0)
                def _(k=k):
                    send_own(k, n_groups // 2, 0, mx_final[k])

            else:
                is_last = b == n_batches - 1 and h == batch - 1
                send_own(k, n_groups // 2 + b, h, mx_final[k], PIECE - EARLY if is_last else PIECE)

    for k in range(n_pieces):
        a, c = divmod(k, share)
        fac[a, pl.ds(c * tiles, tiles), :] = mx_final[k]

    def landed(way, hop, pair):
        ref = out.at[0, pl.ds(0, rows), pl.ds(0, 4 * PIECE)]
        pltpu.make_async_copy(ref, ref, ring_recv.at[way, hop * 2 + pair]).wait()

    def onward(way, hop, pair):
        for i in (2 * pair, 2 * pair + 1):
            g = turn(i)
            ring_copy(way, hop + 1, i, g).start()
            pair_copy(way, hop + 1, g).start()

    for way in (CW, CCW):
        landed(way, 0, 0)
        onward(way, 0, 0)

    recip = 1.0 / mx_final[last]
    for way in (CW, CCW):
        ref = out.at[0, pl.ds(0, rows - rows * EARLY // (4 * PIECE)), pl.ds(0, 4 * PIECE)]
        pltpu.make_async_copy(ref, ref, ring_recv.at[way, 1]).wait()
        pltpu.make_async_copy(early.at[way], early.at[way], early_recv.at[way]).wait()
        owner = lax.rem(chip + (chips - 1 if way == CW else 1), chips) * 2 + core
        rows_of = pl.ds(pl.multiple_of(owner * rows, rows), rows)
        for t in range(EARLY // LANES):
            column = (last % share) * PIECE + PIECE - EARLY + t * LANES
            factor = recip[tiles - EARLY // LANES + t : tiles - EARLY // LANES + t + 1]
            scaled = early[way, :, pl.ds(t * LANES, LANES)] * factor
            out[last // share, rows_of, pl.ds(pl.multiple_of(column, LANES), LANES)] = scaled.astype(jnp.bfloat16)
        onward(way, 0, 1)

    for pair in range(2):
        for way in (CW, CCW):
            landed(way, 1, pair)
            onward(way, 1, pair)

    end = n_groups - 1

    def handover(way):
        ref = part(way, 3, turn(end), 0, 2 * PIECE)
        return pltpu.make_async_remote_copy(
            src_ref=ref, dst_ref=ref, send_sem=ring_send, recv_sem=hand_recv.at[way], device_id=partner,
            device_id_type=MESH,
        )

    def relayed(way, hop):
        owner = lax.rem(chip + (2 * chips - hop if way == CW else hop), chips) * 2 + 1 - core
        g = lax.rem(end + (1 - core) * (n_groups // 2), n_groups)
        start = (g % (n_groups // 2)) * (2 * PIECE) + way * PIECE
        rows_of = pl.ds(pl.multiple_of(owner * rows, rows), rows)
        return out.at[g // (n_groups // 2), rows_of, pl.ds(pl.multiple_of(start, PIECE), PIECE)]

    def relay(way):
        ref = relayed(way, 3)
        return pltpu.make_async_remote_copy(
            src_ref=ref, dst_ref=ref, send_sem=ring_send, recv_sem=relay_recv.at[way],
            device_id=peer(1 if way == CW else -1), device_id_type=MESH,
        )

    def relay_back(way):
        ref = relayed(way, 4)
        return pltpu.make_async_remote_copy(
            src_ref=ref, dst_ref=ref, send_sem=ring_send, recv_sem=pair_recv, device_id=partner, device_id_type=MESH
        )

    for pair in range(2):
        for way in (CW, CCW):
            landed(way, 2, pair)
            for i in (2 * pair, 2 * pair + 1):
                g = turn(i)
                if i < end:
                    ring_copy(way, 3, i, g, way * PIECE, PIECE).start()
                    pair_copy(way, 3, g).start()
                else:
                    handover(way).start()

                    @pl.when(core == 1)
                    def _(way=way, i=i, g=g):
                        ring_copy(way, 3, i, g, way * PIECE, PIECE).start()

    @pl.when(core == 1)
    def _():
        for way in (CW, CCW):
            handover(way).wait_recv()
            relay(way).start()

    def fourth(i, _):
        g = turn(i)
        for way in (CW, CCW):
            ring_copy(way, 3, i, g, way * PIECE, PIECE).wait_recv()
            pair_copy(way, 4, g, way * PIECE, PIECE).start()
        return 0

    lax.fori_loop(0, end, fourth, 0)

    @pl.when(core == 1)
    def _():
        fourth(end, 0)
        for way in (CW, CCW):
            relay(way).wait_recv()
            relay_back(way).start()


    last_rows = rows * PIECE // cols
    for this, sign in ((0, -1), (1, 1)):

        @pl.when(core == this)
        def _(this=this, sign=sign):
            handed = out.at[:, pl.ds(0, chips * rows - 2 * last_rows - sign * last_rows)]
            pltpu.make_async_copy(handed, handed, pair_recv).wait()
            if this == 0:
                for way in (CW, CCW):
                    handover(way).wait_recv()
            sent = out.at[:, pl.ds(0, (2 * chips - 1) * rows - rows * EARLY // cols + sign * 2 * last_rows)]
            pltpu.make_async_copy(sent, sent, ring_send).wait()

    pltpu.make_async_copy(early, early, early_send).wait()
    pltpu.make_async_copy(mx_first, mx_first, first_send).wait()
    pltpu.make_async_copy(mx_all, mx_all, mx_send).wait()
    pltpu.make_async_copy(mx_pair, mx_pair, final_send).wait()


def write_kernel(full, fac, gate, up, fac_gate, fac_up, sem):
    step = full.shape[1] // 4
    smalls = [pltpu.make_async_copy(fac.at[a], dst, sem.at[2 + a]) for a, dst in enumerate((fac_gate, fac_up))]
    for a, dst in enumerate((gate, up)):
        for i in range(4):
            span = pl.ds(i * step, step)
            pltpu.make_async_copy(full.at[a, span], dst.at[span], sem.at[a]).start()
    for small in smalls:
        small.start()
    for a, dst in enumerate((gate, up)):
        pltpu.make_async_copy(full.at[a], dst, sem.at[a]).wait()
    for small in smalls:
        small.wait()


def per_device(weight_gate, moment_gate, square_gate, weight_up, moment_up, square_up, norm_gain):
    rows, cols = weight_gate.shape
    n = lax.axis_size("zero")
    chips = n // 2
    n_pieces = 2 * cols // PIECE
    tiles = PIECE // LANES
    hbm = pl.BlockSpec(memory_space=pltpu.HBM)
    vmem = pl.BlockSpec(memory_space=pltpu.VMEM)
    stored = (weight_gate, moment_gate, square_gate, weight_up, moment_up, square_up, norm_gain.reshape(1, rows))
    stored = tuple(pltpu.with_memory_space_constraint(x, pltpu.HBM) for x in stored)
    full, fac = pl.pallas_call(
        gather_kernel,
        name="ring",
        out_shape=(
            pltpu.VMEM((2, n * rows, cols), jnp.bfloat16),
            pltpu.VMEM((2, cols // LANES, LANES), jnp.float32),
        ),
        in_specs=[hbm] * 7,
        out_specs=(vmem, vmem),
        scratch_shapes=[
            pltpu.VMEM((3, rows, 2 * cols), jnp.float32),
            pltpu.VMEM((1, rows), jnp.float32),
            pltpu.VMEM((rows, rows), jnp.float32),
            pltpu.VMEM((n_pieces, tiles, LANES), jnp.float32),
            pltpu.VMEM((n_pieces // 2, tiles, LANES), jnp.float32),
            pltpu.VMEM((n_pieces // 2, tiles, LANES), jnp.float32),
            pltpu.VMEM((chips - 1, n_pieces // 2, tiles, LANES), jnp.float32),
            pltpu.VMEM((n - 1, tiles, LANES), jnp.float32),
            pltpu.VMEM((n_pieces, tiles, LANES), jnp.float32),
            pltpu.VMEM((2, rows, EARLY), jnp.float32),
            pltpu.SemaphoreType.DMA((n_pieces,)),
            pltpu.SemaphoreType.DMA,
            pltpu.SemaphoreType.DMA,
            pltpu.SemaphoreType.DMA((2, 10)),
            pltpu.SemaphoreType.DMA,
            pltpu.SemaphoreType.DMA,
            pltpu.SemaphoreType.DMA,
            pltpu.SemaphoreType.DMA,
            pltpu.SemaphoreType.DMA((2,)),
            pltpu.SemaphoreType.DMA,
            pltpu.SemaphoreType.DMA,
            pltpu.SemaphoreType.DMA,
            pltpu.SemaphoreType.DMA((2,)),
            pltpu.SemaphoreType.DMA,
            pltpu.SemaphoreType.DMA((2,)),
            pltpu.SemaphoreType.DMA((2,)),
            pltpu.SemaphoreType.DMA((2,)),
        ],
        compiler_params=pltpu.CompilerParams(
            collective_id=0, has_side_effects=True, vmem_limit_bytes=16 * 1024 * 1024
        ),
    )(*stored)
    full, fac = (pltpu.with_memory_space_constraint(x, pltpu.VMEM) for x in (full, fac))
    gate, up, fac_gate, fac_up = pl.pallas_call(
        write_kernel,
        name="write",
        out_shape=(
            jax.ShapeDtypeStruct((n * rows, cols), jnp.bfloat16),
            jax.ShapeDtypeStruct((n * rows, cols), jnp.bfloat16),
            jax.ShapeDtypeStruct((cols // LANES, LANES), jnp.float32),
            jax.ShapeDtypeStruct((cols // LANES, LANES), jnp.float32),
        ),
        in_specs=[pl.BlockSpec(memory_space=pl.ANY)] * 2,
        out_specs=(hbm,) * 4,
        scratch_shapes=[pltpu.SemaphoreType.DMA((4,))],
        compiler_params=pltpu.CompilerParams(vmem_limit_bytes=1024 * 1024),
    )(full, fac)
    return gate, up, fac_gate.reshape(cols), fac_up.reshape(cols)


def solution(mesh):
    placed = (P(("ens", "zero"), "cols"),) * 6 + (P(("ens", "zero")),)
    return jax.shard_map(
        per_device,
        mesh=mesh,
        in_specs=placed,
        out_specs=(P("ens", "cols"), P("ens", "cols"), P(("ens", "cols")), P(("ens", "cols"))),
        check_vma=False,
    )
```

```python
import jax
import jax.numpy as jnp
from jax import lax
from jax.experimental import pallas as pl
from jax.experimental.pallas import tpu as pltpu
from jax.sharding import PartitionSpec as P

learn_rate = 0.2
hold_rate = 0.9
MESH = pl.DeviceIdType.MESH
LANES = 128
PIECE = 512
LAST = 128
EARLY = 256
CW, CCW = 0, 1


def gather_kernel(
    wg, mg, sg, wu, mu, su, gain_hbm, out, fac,
    buf, gain_row, gain_b, mx_own, mx_pair, mx_comb, mx_all, mx_first, mx_final, early,
    load_sem, gain_sem, ring_send, ring_recv, pair_recv, mxp_send, mxp_recv, mx_send, mx_recv,
    first_send, first_recv, final_send, final_recv, early_send, early_recv, hand_recv, relay_recv,
):
    rows, cols = wg.shape
    n_pieces = 2 * cols // PIECE
    tiles = PIECE // LANES
    chips = lax.axis_size("zero") // 2
    far_first = (4, 3, 5, 2, 6, 1, 7)

    me = lax.axis_index("zero")
    chip, core = me // 2, me % 2

    def peer(step, other=False):
        c = 1 - core if other else core
        return {"zero": lax.rem(chip + step + 2 * chips, chips) * 2 + c}

    partner = peer(0, True)

    n_groups = n_pieces // 2

    def loads(k):
        a, c = divmod(k, n_pieces // 2)
        span = pl.ds(c * PIECE, PIECE)
        dst = pl.ds(k * PIECE, PIECE)
        srcs = ((wg, mg, sg), (wu, mu, su))[a]
        return [
            pltpu.make_async_copy(src.at[:, span], buf.at[i, :, dst], load_sem.at[k])
            for i, src in enumerate(srcs)
        ]

    gain_copy = pltpu.make_async_copy(gain_hbm, gain_row, gain_sem)
    gain_copy.start()
    for k in range(n_pieces):
        for copy in loads(k):
            copy.start()

    barrier = pltpu.get_barrier_semaphore()
    for step in far_first:
        for other in (False, True):
            pl.semaphore_signal(barrier, inc=1, device_id=peer(step, other), device_id_type=MESH)
    pl.semaphore_signal(barrier, inc=1, device_id=partner, device_id_type=MESH)

    gain_copy.wait()
    gain_b[...] = jnp.broadcast_to(gain_row[...], (rows, rows)).T

    for k in range(n_pieces):
        landed = buf.at[:, :, pl.ds(k * PIECE, PIECE)]
        pltpu.make_async_copy(landed, landed, load_sem.at[k]).wait()
        for t in range(tiles):
            span = pl.ds(k * PIECE + t * LANES, LANES)
            hold = hold_rate * buf[1, :, span] + buf[2, :, span]
            gained = (buf[0, :, span] - learn_rate * hold) * gain_b[...]
            buf[0, :, span] = gained
            mx_own[k, pl.ds(t, 1), :] = jnp.max(jnp.abs(gained), axis=0, keepdims=True)

    pl.semaphore_wait(barrier, 2 * chips - 1)

    share = n_pieces // 2
    mine, theirs = core * share, (1 - core) * share
    pair_max = pltpu.make_async_remote_copy(
        src_ref=mx_own.at[pl.ds(theirs, share)], dst_ref=mx_pair, send_sem=mxp_send, recv_sem=mxp_recv,
        device_id=partner, device_id_type=MESH,
    )
    pair_max.start()

    def first_copy(step, other):
        slot = 2 * step + (1 if other else 0) - 1
        return pltpu.make_async_remote_copy(
            src_ref=mx_own.at[0], dst_ref=mx_first.at[slot], send_sem=first_send,
            recv_sem=first_recv, device_id=peer(step, other), device_id_type=MESH,
        )

    direct = [(step, other) for step in far_first for other in (False, True)] + [(0, True)]
    for step, other in direct:
        first_copy(step, other).start()

    last = theirs + share - 1
    early_from = pl.multiple_of(last * PIECE + PIECE - EARLY, LANES)

    def early_copy(way, start, size):
        span = pl.ds(start, size)
        return pltpu.make_async_remote_copy(
            src_ref=buf.at[0, span, pl.ds(early_from, EARLY)], dst_ref=early.at[way, span], send_sem=early_send,
            recv_sem=early_recv.at[way], device_id=peer(1 if way == CW else -1), device_id_type=MESH,
        )

    for way in (CW, CCW):
        early_copy(way, 0, 64).start()

    pair_max.wait()
    mx_comb[...] = jnp.maximum(mx_own[pl.ds(mine, share)], mx_pair[...])
    batch = 2
    n_batches = share // batch

    def max_copy(b, step):
        span = pl.ds(b * batch, batch)
        return pltpu.make_async_remote_copy(
            src_ref=mx_comb.at[span], dst_ref=mx_all.at[step - 1, span], send_sem=mx_send,
            recv_sem=mx_recv.at[b], device_id=peer(step), device_id_type=MESH,
        )

    for b in range(n_batches):
        for step in far_first:
            max_copy(b, step).start()
    for way in (CW, CCW):
        early_copy(way, 64, rows - 64).start()

    def part(way, hop, g, start, width):
        owner = lax.rem(chip + (2 * chips - hop if way == CW else hop), chips) * 2 + core
        start = (g % (n_groups // 2)) * (2 * PIECE) + start
        rows_of = pl.ds(pl.multiple_of(owner * rows, rows), rows)
        return out.at[g // (n_groups // 2), rows_of, pl.ds(pl.multiple_of(start, LANES), width)]

    def ring_copy(way, hop, i, g, start=0, width=2 * PIECE):
        ref = part(way, hop, g, start, width)
        slot = hop * 2 + i // 2 if width == 2 * PIECE or hop == 0 else 6 + i
        return pltpu.make_async_remote_copy(
            src_ref=ref, dst_ref=ref, send_sem=ring_send, recv_sem=ring_recv.at[way, slot],
            device_id=peer(1 if way == CW else -1), device_id_type=MESH,
        )

    def pair_copy(way, hop, g, start=0, width=2 * PIECE):
        ref = part(way, hop, g, start, width)
        return pltpu.make_async_remote_copy(
            src_ref=ref, dst_ref=ref, send_sem=ring_send, recv_sem=pair_recv, device_id=partner, device_id_type=MESH
        )

    def turn(i):
        return lax.rem(i + core * (n_groups // 2), n_groups)

    def send_own(k, i, half, top, width=PIECE):
        recip = 1.0 / top
        a, c = k // share, k % share
        for t in range(tiles):
            src = pl.ds(pl.multiple_of(k * PIECE + t * LANES, LANES), LANES)
            dst = pl.ds(pl.multiple_of(c * PIECE + t * LANES, LANES), LANES)
            rows_of = pl.ds(pl.multiple_of(me * rows, rows), rows)
            out[a, rows_of, dst] = (buf[0, :, src] * recip[t : t + 1]).astype(jnp.bfloat16)
        g = k // 2
        ring_copy(CW, 0, i, g, half * PIECE, width).start()
        ring_copy(CCW, 0, i, g, half * PIECE, width).start()
        pair_copy(CW, 0, g, half * PIECE, PIECE).start()

    top = mx_own[0]
    pltpu.make_async_copy(mx_first, mx_first, first_recv).wait()
    for slot in range(2 * chips - 1):
        top = jnp.maximum(top, mx_first[slot])
    send_own(0, core * (n_groups // 2), 0, top)

    def final_copy(b):
        ref = mx_final.at[pl.ds(mine + b * batch, batch)]
        return pltpu.make_async_remote_copy(
            src_ref=ref, dst_ref=ref, send_sem=final_send, recv_sem=final_recv.at[b],
            device_id=partner, device_id_type=MESH,
        )

    for b in range(n_batches):
        span = pl.ds(b * batch, batch)
        came = mx_all.at[:, span]
        pltpu.make_async_copy(came, came, mx_recv.at[b]).wait()
        top = mx_comb[span]
        for step in far_first:
            top = jnp.maximum(top, mx_all[step - 1, span])
        mx_final[pl.ds(mine + b * batch, batch)] = top
        final_copy(b).start()
        for h in range(batch):
            if b == 0 and h == 0:

                @pl.when(core == 1)
                def _(top=top[0]):
                    send_own(mine, 0, 0, top)

            else:
                send_own(mine + b * batch + h, b, h, top[h])

    for b in range(n_batches):
        came = mx_final.at[pl.ds(theirs + b * batch, batch)]
        pltpu.make_async_copy(came, came, final_recv.at[b]).wait()
        for h in range(batch):
            k = theirs + b * batch + h
            if b == 0 and h == 0:

                @pl.when(core == 0)
                def _(k=k):
                    send_own(k, n_groups // 2, 0, mx_final[k])

            else:
                is_last = b == n_batches - 1 and h == batch - 1
                send_own(k, n_groups // 2 + b, h, mx_final[k], PIECE - EARLY if is_last else PIECE)

    for k in range(n_pieces):
        a, c = divmod(k, share)
        fac[a, pl.ds(c * tiles, tiles), :] = mx_final[k]

    def landed(way, hop, pair):
        ref = out.at[0, pl.ds(0, rows), pl.ds(0, 4 * PIECE)]
        pltpu.make_async_copy(ref, ref, ring_recv.at[way, hop * 2 + pair]).wait()

    def onward(way, hop, pair):
        for i in (2 * pair, 2 * pair + 1):
            g = turn(i)
            ring_copy(way, hop + 1, i, g).start()
            pair_copy(way, hop + 1, g).start()

    for way in (CW, CCW):
        landed(way, 0, 0)
        onward(way, 0, 0)

    recip = 1.0 / mx_final[last]
    for way in (CW, CCW):
        ref = out.at[0, pl.ds(0, rows - rows * EARLY // (4 * PIECE)), pl.ds(0, 4 * PIECE)]
        pltpu.make_async_copy(ref, ref, ring_recv.at[way, 1]).wait()
        pltpu.make_async_copy(early.at[way], early.at[way], early_recv.at[way]).wait()
        owner = lax.rem(chip + (chips - 1 if way == CW else 1), chips) * 2 + core
        rows_of = pl.ds(pl.multiple_of(owner * rows, rows), rows)
        for t in range(EARLY // LANES):
            column = (last % share) * PIECE + PIECE - EARLY + t * LANES
            factor = recip[tiles - EARLY // LANES + t : tiles - EARLY // LANES + t + 1]
            scaled = early[way, :, pl.ds(t * LANES, LANES)] * factor
            out[last // share, rows_of, pl.ds(pl.multiple_of(column, LANES), LANES)] = scaled.astype(jnp.bfloat16)
        onward(way, 0, 1)

    for pair in range(2):
        for way in (CW, CCW):
            landed(way, 1, pair)
            onward(way, 1, pair)

    end = n_groups - 1

    def handover(way):
        ref = part(way, 3, turn(end), 0, 2 * PIECE)
        return pltpu.make_async_remote_copy(
            src_ref=ref, dst_ref=ref, send_sem=ring_send, recv_sem=hand_recv.at[way], device_id=partner,
            device_id_type=MESH,
        )

    def relayed(way, hop, begin, width):
        owner = lax.rem(chip + (2 * chips - hop if way == CW else hop), chips) * 2 + 1 - core
        g = lax.rem(end + (1 - core) * (n_groups // 2), n_groups)
        start = (g % (n_groups // 2)) * (2 * PIECE) + way * PIECE + begin
        rows_of = pl.ds(pl.multiple_of(owner * rows, rows), rows)
        return out.at[g // (n_groups // 2), rows_of, pl.ds(pl.multiple_of(start, LANES), width)]

    def relay(way):
        ref = relayed(way, 3, 0, PIECE - LAST)
        return pltpu.make_async_remote_copy(
            src_ref=ref, dst_ref=ref, send_sem=ring_send, recv_sem=relay_recv.at[way],
            device_id=peer(1 if way == CW else -1), device_id_type=MESH,
        )

    def relay_end(way, other):
        ref = relayed(way, 3, PIECE - LAST, LAST)
        return pltpu.make_async_remote_copy(
            src_ref=ref, dst_ref=ref, send_sem=ring_send, recv_sem=pair_recv,
            device_id=peer(1 if way == CW else -1, other), device_id_type=MESH,
        )

    def relay_back(way):
        ref = relayed(way, 4, 0, PIECE - LAST)
        return pltpu.make_async_remote_copy(
            src_ref=ref, dst_ref=ref, send_sem=ring_send, recv_sem=pair_recv, device_id=partner, device_id_type=MESH
        )

    for pair in range(2):
        for way in (CW, CCW):
            landed(way, 2, pair)
            for i in (2 * pair, 2 * pair + 1):
                g = turn(i)
                if i < end:
                    ring_copy(way, 3, i, g, way * PIECE, PIECE).start()
                    pair_copy(way, 3, g).start()
                else:
                    handover(way).start()

                    @pl.when(core == 1)
                    def _(way=way, i=i, g=g):
                        ring_copy(way, 3, i, g, way * PIECE, PIECE).start()

    @pl.when(core == 1)
    def _():
        for way in (CW, CCW):
            handover(way).wait_recv()
            relay(way).start()
            relay_end(way, True).start()
            relay_end(way, False).start()

    def fourth(i, _):
        g = turn(i)
        for way in (CW, CCW):
            ring_copy(way, 3, i, g, way * PIECE, PIECE).wait_recv()
            pair_copy(way, 4, g, way * PIECE, PIECE).start()
        return 0

    lax.fori_loop(0, end, fourth, 0)

    @pl.when(core == 1)
    def _():
        fourth(end, 0)
        for way in (CW, CCW):
            relay(way).wait_recv()
            relay_back(way).start()


    last_rows = rows * PIECE // cols
    for this, sign in ((0, -1), (1, 1)):

        @pl.when(core == this)
        def _(this=this, sign=sign):
            ends = rows * LAST // cols if this == 1 else 0
            handed = out.at[:, pl.ds(0, chips * rows - 2 * last_rows - sign * last_rows + ends)]
            pltpu.make_async_copy(handed, handed, pair_recv).wait()
            if this == 0:
                for way in (CW, CCW):
                    handover(way).wait_recv()
            sent = out.at[:, pl.ds(0, (2 * chips - 1) * rows - rows * EARLY // cols + sign * 2 * last_rows)]
            pltpu.make_async_copy(sent, sent, ring_send).wait()

    pltpu.make_async_copy(early, early, early_send).wait()
    pltpu.make_async_copy(mx_first, mx_first, first_send).wait()
    pltpu.make_async_copy(mx_all, mx_all, mx_send).wait()
    pltpu.make_async_copy(mx_pair, mx_pair, final_send).wait()


def write_kernel(full, fac, gate, up, fac_gate, fac_up, sem):
    step = full.shape[1] // 4
    smalls = [pltpu.make_async_copy(fac.at[a], dst, sem.at[2 + a]) for a, dst in enumerate((fac_gate, fac_up))]
    for a, dst in enumerate((gate, up)):
        for i in range(4):
            span = pl.ds(i * step, step)
            pltpu.make_async_copy(full.at[a, span], dst.at[span], sem.at[a]).start()
    for small in smalls:
        small.start()
    for a, dst in enumerate((gate, up)):
        pltpu.make_async_copy(full.at[a], dst, sem.at[a]).wait()
    for small in smalls:
        small.wait()


def per_device(weight_gate, moment_gate, square_gate, weight_up, moment_up, square_up, norm_gain):
    rows, cols = weight_gate.shape
    n = lax.axis_size("zero")
    chips = n // 2
    n_pieces = 2 * cols // PIECE
    tiles = PIECE // LANES
    hbm = pl.BlockSpec(memory_space=pltpu.HBM)
    vmem = pl.BlockSpec(memory_space=pltpu.VMEM)
    stored = (weight_gate, moment_gate, square_gate, weight_up, moment_up, square_up, norm_gain.reshape(1, rows))
    stored = tuple(pltpu.with_memory_space_constraint(x, pltpu.HBM) for x in stored)
    full, fac = pl.pallas_call(
        gather_kernel,
        name="ring",
        out_shape=(
            pltpu.VMEM((2, n * rows, cols), jnp.bfloat16),
            pltpu.VMEM((2, cols // LANES, LANES), jnp.float32),
        ),
        in_specs=[hbm] * 7,
        out_specs=(vmem, vmem),
        scratch_shapes=[
            pltpu.VMEM((3, rows, 2 * cols), jnp.float32),
            pltpu.VMEM((1, rows), jnp.float32),
            pltpu.VMEM((rows, rows), jnp.float32),
            pltpu.VMEM((n_pieces, tiles, LANES), jnp.float32),
            pltpu.VMEM((n_pieces // 2, tiles, LANES), jnp.float32),
            pltpu.VMEM((n_pieces // 2, tiles, LANES), jnp.float32),
            pltpu.VMEM((chips - 1, n_pieces // 2, tiles, LANES), jnp.float32),
            pltpu.VMEM((n - 1, tiles, LANES), jnp.float32),
            pltpu.VMEM((n_pieces, tiles, LANES), jnp.float32),
            pltpu.VMEM((2, rows, EARLY), jnp.float32),
            pltpu.SemaphoreType.DMA((n_pieces,)),
            pltpu.SemaphoreType.DMA,
            pltpu.SemaphoreType.DMA,
            pltpu.SemaphoreType.DMA((2, 10)),
            pltpu.SemaphoreType.DMA,
            pltpu.SemaphoreType.DMA,
            pltpu.SemaphoreType.DMA,
            pltpu.SemaphoreType.DMA,
            pltpu.SemaphoreType.DMA((2,)),
            pltpu.SemaphoreType.DMA,
            pltpu.SemaphoreType.DMA,
            pltpu.SemaphoreType.DMA,
            pltpu.SemaphoreType.DMA((2,)),
            pltpu.SemaphoreType.DMA,
            pltpu.SemaphoreType.DMA((2,)),
            pltpu.SemaphoreType.DMA((2,)),
            pltpu.SemaphoreType.DMA((2,)),
        ],
        compiler_params=pltpu.CompilerParams(
            collective_id=0, has_side_effects=True, vmem_limit_bytes=16 * 1024 * 1024
        ),
    )(*stored)
    full, fac = (pltpu.with_memory_space_constraint(x, pltpu.VMEM) for x in (full, fac))
    gate, up, fac_gate, fac_up = pl.pallas_call(
        write_kernel,
        name="write",
        out_shape=(
            jax.ShapeDtypeStruct((n * rows, cols), jnp.bfloat16),
            jax.ShapeDtypeStruct((n * rows, cols), jnp.bfloat16),
            jax.ShapeDtypeStruct((cols // LANES, LANES), jnp.float32),
            jax.ShapeDtypeStruct((cols // LANES, LANES), jnp.float32),
        ),
        in_specs=[pl.BlockSpec(memory_space=pl.ANY)] * 2,
        out_specs=(hbm,) * 4,
        scratch_shapes=[pltpu.SemaphoreType.DMA((4,))],
        compiler_params=pltpu.CompilerParams(vmem_limit_bytes=1024 * 1024),
    )(full, fac)
    return gate, up, fac_gate.reshape(cols), fac_up.reshape(cols)


def solution(mesh):
    placed = (P(("ens", "zero"), "cols"),) * 6 + (P(("ens", "zero")),)
    return jax.shard_map(
        per_device,
        mesh=mesh,
        in_specs=placed,
        out_specs=(P("ens", "cols"), P("ens", "cols"), P(("ens", "cols")), P(("ens", "cols"))),
        check_vma=False,
    )
```

```python
import jax
import jax.numpy as jnp
from jax import lax
from jax.experimental import pallas as pl
from jax.experimental.pallas import tpu as pltpu
from jax.sharding import PartitionSpec as P

learn_rate = 0.2
hold_rate = 0.9
MESH = pl.DeviceIdType.MESH
LANES = 128
PIECE = 512
LAST = 256
EARLY = 256
CW, CCW = 0, 1


def gather_kernel(
    wg, mg, sg, wu, mu, su, gain_hbm, out, fac,
    buf, gain_row, gain_b, mx_own, mx_pair, mx_comb, mx_all, mx_first, mx_final, early,
    load_sem, gain_sem, ring_send, ring_recv, pair_recv, mxp_send, mxp_recv, mx_send, mx_recv,
    first_send, first_recv, final_send, final_recv, early_send, early_recv, hand_recv, relay_recv,
):
    rows, cols = wg.shape
    n_pieces = 2 * cols // PIECE
    tiles = PIECE // LANES
    chips = lax.axis_size("zero") // 2
    far_first = (4, 3, 5, 2, 6, 1, 7)

    me = lax.axis_index("zero")
    chip, core = me // 2, me % 2

    def peer(step, other=False):
        c = 1 - core if other else core
        return {"zero": lax.rem(chip + step + 2 * chips, chips) * 2 + c}

    partner = peer(0, True)

    n_groups = n_pieces // 2

    def loads(k):
        a, c = divmod(k, n_pieces // 2)
        span = pl.ds(c * PIECE, PIECE)
        dst = pl.ds(k * PIECE, PIECE)
        srcs = ((wg, mg, sg), (wu, mu, su))[a]
        return [
            pltpu.make_async_copy(src.at[:, span], buf.at[i, :, dst], load_sem.at[k])
            for i, src in enumerate(srcs)
        ]

    gain_copy = pltpu.make_async_copy(gain_hbm, gain_row, gain_sem)
    gain_copy.start()
    for k in range(n_pieces):
        for copy in loads(k):
            copy.start()

    barrier = pltpu.get_barrier_semaphore()
    for step in far_first:
        for other in (False, True):
            pl.semaphore_signal(barrier, inc=1, device_id=peer(step, other), device_id_type=MESH)
    pl.semaphore_signal(barrier, inc=1, device_id=partner, device_id_type=MESH)

    gain_copy.wait()
    gain_b[...] = jnp.broadcast_to(gain_row[...], (rows, rows)).T

    for k in range(n_pieces):
        landed = buf.at[:, :, pl.ds(k * PIECE, PIECE)]
        pltpu.make_async_copy(landed, landed, load_sem.at[k]).wait()
        for t in range(tiles):
            span = pl.ds(k * PIECE + t * LANES, LANES)
            hold = hold_rate * buf[1, :, span] + buf[2, :, span]
            gained = (buf[0, :, span] - learn_rate * hold) * gain_b[...]
            buf[0, :, span] = gained
            mx_own[k, pl.ds(t, 1), :] = jnp.max(jnp.abs(gained), axis=0, keepdims=True)

    pl.semaphore_wait(barrier, 2 * chips - 1)

    share = n_pieces // 2
    mine, theirs = core * share, (1 - core) * share
    pair_max = pltpu.make_async_remote_copy(
        src_ref=mx_own.at[pl.ds(theirs, share)], dst_ref=mx_pair, send_sem=mxp_send, recv_sem=mxp_recv,
        device_id=partner, device_id_type=MESH,
    )
    pair_max.start()

    def first_copy(step, other):
        slot = 2 * step + (1 if other else 0) - 1
        return pltpu.make_async_remote_copy(
            src_ref=mx_own.at[0], dst_ref=mx_first.at[slot], send_sem=first_send,
            recv_sem=first_recv, device_id=peer(step, other), device_id_type=MESH,
        )

    direct = [(step, other) for step in far_first for other in (False, True)] + [(0, True)]
    for step, other in direct:
        first_copy(step, other).start()

    last = theirs + share - 1
    early_from = pl.multiple_of(last * PIECE + PIECE - EARLY, LANES)

    def early_copy(way, start, size):
        span = pl.ds(start, size)
        return pltpu.make_async_remote_copy(
            src_ref=buf.at[0, span, pl.ds(early_from, EARLY)], dst_ref=early.at[way, span], send_sem=early_send,
            recv_sem=early_recv.at[way], device_id=peer(1 if way == CW else -1), device_id_type=MESH,
        )

    for way in (CW, CCW):
        early_copy(way, 0, 64).start()

    pair_max.wait()
    mx_comb[...] = jnp.maximum(mx_own[pl.ds(mine, share)], mx_pair[...])
    batch = 2
    n_batches = share // batch

    def max_copy(b, step):
        span = pl.ds(b * batch, batch)
        return pltpu.make_async_remote_copy(
            src_ref=mx_comb.at[span], dst_ref=mx_all.at[step - 1, span], send_sem=mx_send,
            recv_sem=mx_recv.at[b], device_id=peer(step), device_id_type=MESH,
        )

    for b in range(n_batches):
        for step in far_first:
            max_copy(b, step).start()
    for way in (CW, CCW):
        early_copy(way, 64, rows - 64).start()

    def part(way, hop, g, start, width):
        owner = lax.rem(chip + (2 * chips - hop if way == CW else hop), chips) * 2 + core
        start = (g % (n_groups // 2)) * (2 * PIECE) + start
        rows_of = pl.ds(pl.multiple_of(owner * rows, rows), rows)
        return out.at[g // (n_groups // 2), rows_of, pl.ds(pl.multiple_of(start, LANES), width)]

    def ring_copy(way, hop, i, g, start=0, width=2 * PIECE):
        ref = part(way, hop, g, start, width)
        slot = hop * 2 + i // 2 if width == 2 * PIECE or hop == 0 else 6 + i
        return pltpu.make_async_remote_copy(
            src_ref=ref, dst_ref=ref, send_sem=ring_send, recv_sem=ring_recv.at[way, slot],
            device_id=peer(1 if way == CW else -1), device_id_type=MESH,
        )

    def pair_copy(way, hop, g, start=0, width=2 * PIECE):
        ref = part(way, hop, g, start, width)
        return pltpu.make_async_remote_copy(
            src_ref=ref, dst_ref=ref, send_sem=ring_send, recv_sem=pair_recv, device_id=partner, device_id_type=MESH
        )

    def turn(i):
        return lax.rem(i + core * (n_groups // 2), n_groups)

    def send_own(k, i, half, top, width=PIECE):
        recip = 1.0 / top
        a, c = k // share, k % share
        for t in range(tiles):
            src = pl.ds(pl.multiple_of(k * PIECE + t * LANES, LANES), LANES)
            dst = pl.ds(pl.multiple_of(c * PIECE + t * LANES, LANES), LANES)
            rows_of = pl.ds(pl.multiple_of(me * rows, rows), rows)
            out[a, rows_of, dst] = (buf[0, :, src] * recip[t : t + 1]).astype(jnp.bfloat16)
        g = k // 2
        ring_copy(CW, 0, i, g, half * PIECE, width).start()
        ring_copy(CCW, 0, i, g, half * PIECE, width).start()
        pair_copy(CW, 0, g, half * PIECE, PIECE).start()

    top = mx_own[0]
    pltpu.make_async_copy(mx_first, mx_first, first_recv).wait()
    for slot in range(2 * chips - 1):
        top = jnp.maximum(top, mx_first[slot])
    send_own(0, core * (n_groups // 2), 0, top)

    def final_copy(b):
        ref = mx_final.at[pl.ds(mine + b * batch, batch)]
        return pltpu.make_async_remote_copy(
            src_ref=ref, dst_ref=ref, send_sem=final_send, recv_sem=final_recv.at[b],
            device_id=partner, device_id_type=MESH,
        )

    for b in range(n_batches):
        span = pl.ds(b * batch, batch)
        came = mx_all.at[:, span]
        pltpu.make_async_copy(came, came, mx_recv.at[b]).wait()
        top = mx_comb[span]
        for step in far_first:
            top = jnp.maximum(top, mx_all[step - 1, span])
        mx_final[pl.ds(mine + b * batch, batch)] = top
        final_copy(b).start()
        for h in range(batch):
            if b == 0 and h == 0:

                @pl.when(core == 1)
                def _(top=top[0]):
                    send_own(mine, 0, 0, top)

            else:
                send_own(mine + b * batch + h, b, h, top[h])

    for b in range(n_batches):
        came = mx_final.at[pl.ds(theirs + b * batch, batch)]
        pltpu.make_async_copy(came, came, final_recv.at[b]).wait()
        for h in range(batch):
            k = theirs + b * batch + h
            if b == 0 and h == 0:

                @pl.when(core == 0)
                def _(k=k):
                    send_own(k, n_groups // 2, 0, mx_final[k])

            else:
                is_last = b == n_batches - 1 and h == batch - 1
                send_own(k, n_groups // 2 + b, h, mx_final[k], PIECE - EARLY if is_last else PIECE)

    for k in range(n_pieces):
        a, c = divmod(k, share)
        fac[a, pl.ds(c * tiles, tiles), :] = mx_final[k]

    def landed(way, hop, pair):
        ref = out.at[0, pl.ds(0, rows), pl.ds(0, 4 * PIECE)]
        pltpu.make_async_copy(ref, ref, ring_recv.at[way, hop * 2 + pair]).wait()

    def onward(way, hop, pair):
        for i in (2 * pair, 2 * pair + 1):
            g = turn(i)
            ring_copy(way, hop + 1, i, g).start()
            pair_copy(way, hop + 1, g).start()

    for way in (CW, CCW):
        landed(way, 0, 0)
        onward(way, 0, 0)

    recip = 1.0 / mx_final[last]
    for way in (CW, CCW):
        ref = out.at[0, pl.ds(0, rows - rows * EARLY // (4 * PIECE)), pl.ds(0, 4 * PIECE)]
        pltpu.make_async_copy(ref, ref, ring_recv.at[way, 1]).wait()
        pltpu.make_async_copy(early.at[way], early.at[way], early_recv.at[way]).wait()
        owner = lax.rem(chip + (chips - 1 if way == CW else 1), chips) * 2 + core
        rows_of = pl.ds(pl.multiple_of(owner * rows, rows), rows)
        for t in range(EARLY // LANES):
            column = (last % share) * PIECE + PIECE - EARLY + t * LANES
            factor = recip[tiles - EARLY // LANES + t : tiles - EARLY // LANES + t + 1]
            scaled = early[way, :, pl.ds(t * LANES, LANES)] * factor
            out[last // share, rows_of, pl.ds(pl.multiple_of(column, LANES), LANES)] = scaled.astype(jnp.bfloat16)
        onward(way, 0, 1)

    for pair in range(2):
        for way in (CW, CCW):
            landed(way, 1, pair)
            onward(way, 1, pair)

    end = n_groups - 1

    def handover(way):
        ref = part(way, 3, turn(end), 0, 2 * PIECE)
        return pltpu.make_async_remote_copy(
            src_ref=ref, dst_ref=ref, send_sem=ring_send, recv_sem=hand_recv.at[way], device_id=partner,
            device_id_type=MESH,
        )

    def relayed(way, hop, begin, width):
        owner = lax.rem(chip + (2 * chips - hop if way == CW else hop), chips) * 2 + 1 - core
        g = lax.rem(end + (1 - core) * (n_groups // 2), n_groups)
        start = (g % (n_groups // 2)) * (2 * PIECE) + way * PIECE + begin
        rows_of = pl.ds(pl.multiple_of(owner * rows, rows), rows)
        return out.at[g // (n_groups // 2), rows_of, pl.ds(pl.multiple_of(start, LANES), width)]

    def relay(way):
        ref = relayed(way, 3, 0, PIECE - LAST)
        return pltpu.make_async_remote_copy(
            src_ref=ref, dst_ref=ref, send_sem=ring_send, recv_sem=relay_recv.at[way],
            device_id=peer(1 if way == CW else -1), device_id_type=MESH,
        )

    def relay_end(way, other):
        ref = relayed(way, 3, PIECE - LAST, LAST)
        return pltpu.make_async_remote_copy(
            src_ref=ref, dst_ref=ref, send_sem=ring_send, recv_sem=pair_recv,
            device_id=peer(1 if way == CW else -1, other), device_id_type=MESH,
        )

    def relay_back(way):
        ref = relayed(way, 4, 0, PIECE - LAST)
        return pltpu.make_async_remote_copy(
            src_ref=ref, dst_ref=ref, send_sem=ring_send, recv_sem=pair_recv, device_id=partner, device_id_type=MESH
        )

    for pair in range(2):
        for way in (CW, CCW):
            landed(way, 2, pair)
            for i in (2 * pair, 2 * pair + 1):
                g = turn(i)
                if i < end:
                    ring_copy(way, 3, i, g, way * PIECE, PIECE).start()
                    pair_copy(way, 3, g).start()
                else:
                    handover(way).start()

                    @pl.when(core == 1)
                    def _(way=way, i=i, g=g):
                        ring_copy(way, 3, i, g, way * PIECE, PIECE).start()

    @pl.when(core == 1)
    def _():
        for way in (CW, CCW):
            handover(way).wait_recv()
            relay(way).start()
            relay_end(way, True).start()
            relay_end(way, False).start()

    def fourth(i, _):
        g = turn(i)
        for way in (CW, CCW):
            ring_copy(way, 3, i, g, way * PIECE, PIECE).wait_recv()
            pair_copy(way, 4, g, way * PIECE, PIECE).start()
        return 0

    lax.fori_loop(0, end, fourth, 0)

    @pl.when(core == 1)
    def _():
        fourth(end, 0)
        for way in (CW, CCW):
            relay(way).wait_recv()
            relay_back(way).start()


    last_rows = rows * PIECE // cols
    for this, sign in ((0, -1), (1, 1)):

        @pl.when(core == this)
        def _(this=this, sign=sign):
            ends = rows * LAST // cols if this == 1 else 0
            handed = out.at[:, pl.ds(0, chips * rows - 2 * last_rows - sign * last_rows + ends)]
            pltpu.make_async_copy(handed, handed, pair_recv).wait()
            if this == 0:
                for way in (CW, CCW):
                    handover(way).wait_recv()
            sent = out.at[:, pl.ds(0, (2 * chips - 1) * rows - rows * EARLY // cols + sign * 2 * last_rows)]
            pltpu.make_async_copy(sent, sent, ring_send).wait()

    pltpu.make_async_copy(early, early, early_send).wait()
    pltpu.make_async_copy(mx_first, mx_first, first_send).wait()
    pltpu.make_async_copy(mx_all, mx_all, mx_send).wait()
    pltpu.make_async_copy(mx_pair, mx_pair, final_send).wait()


def write_kernel(full, fac, gate, up, fac_gate, fac_up, sem):
    step = full.shape[1] // 4
    smalls = [pltpu.make_async_copy(fac.at[a], dst, sem.at[2 + a]) for a, dst in enumerate((fac_gate, fac_up))]
    for a, dst in enumerate((gate, up)):
        for i in range(4):
            span = pl.ds(i * step, step)
            pltpu.make_async_copy(full.at[a, span], dst.at[span], sem.at[a]).start()
    for small in smalls:
        small.start()
    for a, dst in enumerate((gate, up)):
        pltpu.make_async_copy(full.at[a], dst, sem.at[a]).wait()
    for small in smalls:
        small.wait()


def per_device(weight_gate, moment_gate, square_gate, weight_up, moment_up, square_up, norm_gain):
    rows, cols = weight_gate.shape
    n = lax.axis_size("zero")
    chips = n // 2
    n_pieces = 2 * cols // PIECE
    tiles = PIECE // LANES
    hbm = pl.BlockSpec(memory_space=pltpu.HBM)
    vmem = pl.BlockSpec(memory_space=pltpu.VMEM)
    stored = (weight_gate, moment_gate, square_gate, weight_up, moment_up, square_up, norm_gain.reshape(1, rows))
    stored = tuple(pltpu.with_memory_space_constraint(x, pltpu.HBM) for x in stored)
    full, fac = pl.pallas_call(
        gather_kernel,
        name="ring",
        out_shape=(
            pltpu.VMEM((2, n * rows, cols), jnp.bfloat16),
            pltpu.VMEM((2, cols // LANES, LANES), jnp.float32),
        ),
        in_specs=[hbm] * 7,
        out_specs=(vmem, vmem),
        scratch_shapes=[
            pltpu.VMEM((3, rows, 2 * cols), jnp.float32),
            pltpu.VMEM((1, rows), jnp.float32),
            pltpu.VMEM((rows, rows), jnp.float32),
            pltpu.VMEM((n_pieces, tiles, LANES), jnp.float32),
            pltpu.VMEM((n_pieces // 2, tiles, LANES), jnp.float32),
            pltpu.VMEM((n_pieces // 2, tiles, LANES), jnp.float32),
            pltpu.VMEM((chips - 1, n_pieces // 2, tiles, LANES), jnp.float32),
            pltpu.VMEM((n - 1, tiles, LANES), jnp.float32),
            pltpu.VMEM((n_pieces, tiles, LANES), jnp.float32),
            pltpu.VMEM((2, rows, EARLY), jnp.float32),
            pltpu.SemaphoreType.DMA((n_pieces,)),
            pltpu.SemaphoreType.DMA,
            pltpu.SemaphoreType.DMA,
            pltpu.SemaphoreType.DMA((2, 10)),
            pltpu.SemaphoreType.DMA,
            pltpu.SemaphoreType.DMA,
            pltpu.SemaphoreType.DMA,
            pltpu.SemaphoreType.DMA,
            pltpu.SemaphoreType.DMA((2,)),
            pltpu.SemaphoreType.DMA,
            pltpu.SemaphoreType.DMA,
            pltpu.SemaphoreType.DMA,
            pltpu.SemaphoreType.DMA((2,)),
            pltpu.SemaphoreType.DMA,
            pltpu.SemaphoreType.DMA((2,)),
            pltpu.SemaphoreType.DMA((2,)),
            pltpu.SemaphoreType.DMA((2,)),
        ],
        compiler_params=pltpu.CompilerParams(
            collective_id=0, has_side_effects=True, vmem_limit_bytes=16 * 1024 * 1024
        ),
    )(*stored)
    full, fac = (pltpu.with_memory_space_constraint(x, pltpu.VMEM) for x in (full, fac))
    gate, up, fac_gate, fac_up = pl.pallas_call(
        write_kernel,
        name="write",
        out_shape=(
            jax.ShapeDtypeStruct((n * rows, cols), jnp.bfloat16),
            jax.ShapeDtypeStruct((n * rows, cols), jnp.bfloat16),
            jax.ShapeDtypeStruct((cols // LANES, LANES), jnp.float32),
            jax.ShapeDtypeStruct((cols // LANES, LANES), jnp.float32),
        ),
        in_specs=[pl.BlockSpec(memory_space=pl.ANY)] * 2,
        out_specs=(hbm,) * 4,
        scratch_shapes=[pltpu.SemaphoreType.DMA((4,))],
        compiler_params=pltpu.CompilerParams(vmem_limit_bytes=1024 * 1024),
    )(full, fac)
    return gate, up, fac_gate.reshape(cols), fac_up.reshape(cols)


def solution(mesh):
    placed = (P(("ens", "zero"), "cols"),) * 6 + (P(("ens", "zero")),)
    return jax.shard_map(
        per_device,
        mesh=mesh,
        in_specs=placed,
        out_specs=(P("ens", "cols"), P("ens", "cols"), P(("ens", "cols")), P(("ens", "cols"))),
        check_vma=False,
    )
```
